256 devices in a mesh: sp: 64 (over z, y, core), tp: 4 (over x).
Axes of the slice: x: 4, y: 4, z: 8, core: 2. Of those that a mesh axis runs over, the one named last changes fastest.
Arguments:
- decay_rate: float32 [4, 65536, 1024], P(None, 'sp', 'tp'), may hold values from 0.2 to 2
- drive_in: bfloat16 [4, 65536, 1024], P(None, 'sp', 'tp'), may hold values from -6 to 6
- gate_in: bfloat16 [4, 65536, 1024], P(None, 'sp', 'tp'), may hold values from -6 to 6
- norm_gain: float32 [1024], P('tp'), may hold values from 0.25 to 1.75
Outputs:
- filtered: bfloat16 [4, 65536, 1024], P(None, 'sp', 'tp')
The draws below stay inside these ranges and needn't reach their ends.
All inputs are finite; a program needn't handle non-finite values.
Results may differ from the reference program's by a relative error of at most 0.0015.
Values sent between devices are 32-bit elements.
No kernel may reach another device: no remote copies, remote signals or barrier semaphores. Data moves between devices by JAX's collectives and lax.ppermute only.
A program may use at most 128 MiB of HBM per device.

```python
import jax
import jax.numpy as jnp
from jax import lax

BATCH = 4
CHANNELS = 1024
LENGTH = 65536


def block_scale(stream_key, extent, shards, smallest, high):
    def one(dim, blocks):
        steps = jax.random.uniform(jax.random.fold_in(jax.random.fold_in(stream_key, 6), dim), (blocks,), jnp.float32, smallest / len(shards), high / len(shards))
        return jnp.repeat(jnp.exp(steps), extent[dim] // blocks).reshape((-1,) + (1,) * (len(extent) - dim - 1))

    factor_of = one(*shards[0])
    for cut in shards[1:]:
        factor_of = factor_of * one(*cut)
    return factor_of


def gaussian(stream_key, dims, width, reach, pieces=(), held_as=jnp.bfloat16):
    array = jax.random.normal(stream_key, dims, jnp.float32) * width
    if len(pieces) > 0:
        array = block_scale(stream_key, dims, pieces, -0.22, 0.18) * array
    return jnp.clip(array, min=-reach, max=reach).astype(held_as)


def setup_inputs(seed: int = 0) -> dict:
    streams_of = jax.random.split(jax.random.key(seed), 5)
    decay_rate = jnp.clip(0.2 + 1.8 * jax.random.uniform(streams_of[0], (BATCH, LENGTH, CHANNELS), jnp.float32) ** block_scale(streams_of[0], (BATCH, LENGTH, CHANNELS), ((1, 64), (2, 4)), -0.2, 0.2), 0.2, 2.0)
    drive_in = gaussian(streams_of[1], (BATCH, LENGTH, CHANNELS), 1.0, 6.0, ((1, 64), (2, 4)))
    gate_in = gaussian(streams_of[2], (BATCH, LENGTH, CHANNELS), 1.0, 6.0, ((1, 64), (2, 4)))
    norm_gain = jnp.clip(1.0 + 0.15 * jax.random.normal(streams_of[3], (CHANNELS,), jnp.float32), 0.25, 1.75)
    return dict(decay_rate=decay_rate, drive_in=drive_in, gate_in=gate_in, norm_gain=norm_gain)


def join_pair(earlier, later):
    return (earlier[0] * later[0], later[0] * earlier[1] + later[1])

def reference(decay_rate, drive_in, gate_in, norm_gain):
    keep = jnp.exp(-decay_rate / LENGTH)
    push = drive_in.astype(jnp.float32) * LENGTH ** (-0.5)
    forward = lax.associative_scan(join_pair, (keep, push), axis=1)[1]
    gated = forward * jax.nn.sigmoid(gate_in.astype(jnp.float32))
    power = lax.optimization_barrier(jnp.mean(gated * gated, axis=-1, keepdims=True))
    filtered = (gated * lax.rsqrt(power + 1e-06) * norm_gain).astype(jnp.bfloat16)
    return filtered
```

```python
import functools

import jax
import jax.numpy as jnp
from jax import lax
from jax.experimental import pallas as pl
from jax.experimental.pallas import tpu as pltpu
from jax.sharding import Mesh
from jax.sharding import PartitionSpec as P

SP = ("sp_0", "sp_1", "sp_2")
BLOCK = 256
MIB = 1 << 20


def triangle():
    row = lax.broadcasted_iota(jnp.int32, (BLOCK, BLOCK), 0)
    col = lax.broadcasted_iota(jnp.int32, (BLOCK, BLOCK), 1)
    return (row >= col).astype(jnp.bfloat16)


def running_sum(tri, x):
    high = x.astype(jnp.bfloat16)
    low = (x - high.astype(jnp.float32)).astype(jnp.bfloat16)
    dot = functools.partial(jnp.dot, preferred_element_type=jnp.float32)
    return dot(tri, high) + dot(tri, low)


def pieces(hbm, vmem, sems):
    batch, length, _ = hbm.shape
    steps = length // BLOCK

    def piece(i):
        b, at = i // steps, pl.ds(pl.multiple_of((i % steps) * BLOCK, BLOCK), BLOCK)
        return pltpu.make_async_copy(hbm.at[b, at, :], vmem.at[b, at, :], sems.at[i])

    return piece


def summary_kernel(total, rate_hbm, drive_hbm, depth_ref, term_ref, out_ref, rate, drive, tri_ref, rate_sem, drive_sem):
    batch, length, channels = rate.shape
    steps = length // BLOCK
    rate_piece, drive_piece = pieces(rate_hbm, rate, rate_sem), pieces(drive_hbm, drive, drive_sem)
    for i in range(batch * steps):
        rate_piece(i).start()
        drive_piece(i).start()
    tri_ref[...] = triangle()
    for b in range(batch):
        depth_in = jnp.zeros((1, channels), jnp.float32)
        sums = jnp.zeros((8, channels), jnp.float32)
        for s in range(steps):
            at = pl.ds(s * BLOCK, BLOCK)
            rate_piece(b * steps + s).wait()
            depth = running_sum(tri_ref[...], rate[b, at, :]) * (1.0 / total) + depth_in
            depth_ref[b, at, :] = depth
            depth_in = depth[BLOCK - 1 :, :]
            drive_piece(b * steps + s).wait()
            term = jnp.exp(depth) * (drive[b, at, :].astype(jnp.float32) * total**-0.5)
            term_ref[b, at, :] = term
            sums = sums + jnp.sum(term.reshape(BLOCK // 8, 8, channels), axis=0)
        out_ref[b : b + 1, :] = depth_in
        out_ref[batch + b : batch + b + 1, :] = jnp.sum(sums, axis=0, keepdims=True)


def summarize(decay_rate, drive_in, total):
    batch, length, channels = decay_rate.shape
    count = batch * length // BLOCK
    big = jax.ShapeDtypeStruct(decay_rate.shape, jnp.float32)
    vmem = pl.BlockSpec(memory_space=pltpu.VMEM)
    return pl.pallas_call(
        functools.partial(summary_kernel, total),
        out_shape=(big, big, jax.ShapeDtypeStruct((2 * batch, channels), jnp.float32)),
        in_specs=[pl.BlockSpec(memory_space=pl.ANY)] * 2,
        out_specs=(vmem, vmem, vmem),
        scratch_shapes=[
            pltpu.VMEM(decay_rate.shape, jnp.float32),
            pltpu.VMEM(drive_in.shape, jnp.bfloat16),
            pltpu.VMEM((BLOCK, BLOCK), jnp.bfloat16),
            pltpu.SemaphoreType.DMA((count,)),
            pltpu.SemaphoreType.DMA((count,)),
        ],
        compiler_params=pltpu.CompilerParams(vmem_limit_bytes=24 * MIB),
        cost_estimate=pl.CostEstimate(flops=2_000_000_000, bytes_accessed=6 * MIB, transcendentals=MIB),
        name="summarize",
    )(decay_rate, drive_in)


def local_kernel(depth_ref, term_ref, gate_hbm, factor_ref, sum_ref, gate, tri_ref, gate_sem):
    batch, length, channels = gate.shape
    steps = length // BLOCK
    gate_piece = pieces(gate_hbm, gate, gate_sem)
    for i in range(batch * steps):
        gate_piece(i).start()
    tri_ref[...] = triangle()
    for b in range(batch):
        carried = jnp.zeros((1, channels), jnp.float32)
        for s in range(steps):
            at = pl.ds(s * BLOCK, BLOCK)
            sums = running_sum(tri_ref[...], term_ref[b, at, :]) + carried
            sum_ref[b, at, :] = sums
            carried = sums[BLOCK - 1 :, :]
            gate_piece(b * steps + s).wait()
            opened = 0.5 * jnp.tanh(0.5 * gate[b, at, :].astype(jnp.float32)) + 0.5
            factor_ref[b, at, :] = jnp.exp(-depth_ref[b, at, :]) * opened


def localize(depth, term, gate_in):
    batch, length, channels = depth.shape
    count = batch * length // BLOCK
    big = jax.ShapeDtypeStruct(depth.shape, jnp.float32)
    vmem = pl.BlockSpec(memory_space=pltpu.VMEM)
    return pl.pallas_call(
        local_kernel,
        out_shape=(big, big),
        in_specs=[vmem, vmem, pl.BlockSpec(memory_space=pl.ANY)],
        out_specs=(vmem, vmem),
        scratch_shapes=[
            pltpu.VMEM(gate_in.shape, jnp.bfloat16),
            pltpu.VMEM((BLOCK, BLOCK), jnp.bfloat16),
            pltpu.SemaphoreType.DMA((count,)),
        ],
        compiler_params=pltpu.CompilerParams(vmem_limit_bytes=24 * MIB),
        cost_estimate=pl.CostEstimate(flops=2_000_000_000, bytes_accessed=2 * MIB, transcendentals=2 * MIB),
        name="localize",
    )(depth, term, gate_in)


def gate_kernel(factor_ref, sum_ref, enter_ref, gated_ref, power_ref):
    batch, length, channels = factor_ref.shape
    lane = lax.broadcasted_iota(jnp.int32, (8, 128), 1)
    for b in range(batch):
        enter = enter_ref[b : b + 1, :]

        def step(j, power):
            at = pl.ds(pl.multiple_of(j * 64, 64), 64)
            gated = factor_ref[b, at, :] * (sum_ref[b, at, :] + enter)
            gated_ref[b, at, :] = gated
            square = gated * gated
            for k in range(8):
                sums = jnp.sum(square[8 * k : 8 * k + 8, :], axis=-1, keepdims=True)
                power = jnp.where(lane == j * 8 + k, sums, power)
            return power

        power_ref[b] = lax.fori_loop(0, length // 64, step, jnp.zeros((8, 128), jnp.float32))


def gate_and_square(factor, sums, enter):
    batch, length, channels = factor.shape
    vmem = pl.BlockSpec(memory_space=pltpu.VMEM)
    return pl.pallas_call(
        gate_kernel,
        out_shape=(jax.ShapeDtypeStruct(factor.shape, jnp.float32), jax.ShapeDtypeStruct((batch, 8, length // 8), jnp.float32)),
        in_specs=[vmem] * 3,
        out_specs=(vmem, vmem),
        compiler_params=pltpu.CompilerParams(vmem_limit_bytes=16 * MIB),
        cost_estimate=pl.CostEstimate(flops=8_000_000, bytes_accessed=12 * MIB, transcendentals=0),
        name="gate_and_square",
    )(factor, sums, enter)


def scale_kernel(width, gated_ref, p0_ref, p1_ref, p2_ref, p3_ref, gain_ref, out_ref):
    batch, length, channels = gated_ref.shape
    gain = gain_ref[...]
    for b in range(batch):
        power = (p0_ref[b] + p1_ref[b]) + (p2_ref[b] + p3_ref[b])
        scale = lax.rsqrt(power * (1.0 / width) + 1e-06)
        for j in range(length // 16):
            at = pl.ds(j * 16, 16)
            rows = jnp.concatenate(
                [jnp.broadcast_to(scale[:, 2 * j + k : 2 * j + k + 1], (8, channels)) for k in range(2)], axis=0
            )
            out_ref[b, at, :] = (gated_ref[b, at, :] * rows * gain).astype(jnp.bfloat16)


def scale(gated, powers, gain, width):
    batch, length, channels = gated.shape
    vmem = pl.BlockSpec(memory_space=pltpu.VMEM)
    return pl.pallas_call(
        functools.partial(scale_kernel, width),
        out_shape=jax.ShapeDtypeStruct(gated.shape, jnp.bfloat16),
        in_specs=[vmem] * 6,
        out_specs=vmem,
        compiler_params=pltpu.CompilerParams(vmem_limit_bytes=16 * MIB),
        cost_estimate=pl.CostEstimate(flops=8_000_000, bytes_accessed=6 * MIB, transcendentals=0),
        name="scale",
    )(gated, *powers, gain.reshape(1, channels))


def join(earlier, later):
    return (earlier[0] + later[0], earlier[1] + jnp.exp(earlier[0]) * later[1])


def split(pair):
    half = pair.shape[0] // 2
    return (pair[:half], pair[half:])


def masked(pair, keep):
    return jnp.where(keep, pair, 0.0)


def entering_state(pair, ways):
    chips_z, chips_y = ways
    core, y = lax.axis_index("sp_2"), lax.axis_index("sp_1")
    first = lax.ppermute(pair, "sp_2", [(0, 1)])
    chip = jnp.concatenate(join(split(first), split(pair)))
    def on_second(axis_pairs):
        return [(2 * a + 1, 2 * b + 1) for a, b in axis_pairs]

    near = {
        k: lax.ppermute(chip, ("sp_1", "sp_2"), on_second([(i, (i + k) % chips_y) for i in range(chips_y)]))
        for k in (2, 3, 1)
    }
    before = split(masked(near[chips_y - 1], y >= chips_y - 1))
    after = split(masked(near[chips_y - 1], y < chips_y - 1))
    for k in range(chips_y - 2, 0, -1):
        before = join(before, split(masked(near[k], y >= k)))
        after = join(after, split(masked(near[k], y < k)))
    plane = jnp.concatenate(join(join(before, split(chip)), after))
    stride = 2 * chips_y
    others = [(c * 2 + 1) for c in range(chips_y)]
    far = {
        k: lax.ppermute(
            plane,
            SP,
            [(i * stride + c, (i + k) * stride + c) for i in range(chips_z - k) for c in others],
        )
        for k in range(chips_z - 1, 0, -1)
    }
    so_far = split(far[chips_z - 1])
    for k in range(chips_z - 2, 0, -1):
        so_far = join(so_far, split(far[k]))
    so_far = join(so_far, before)
    enter = so_far[1] * jnp.exp(-so_far[0])
    own = jnp.exp(-split(first)[0]) * (enter + split(first)[1])
    back = lax.ppermute(enter, "sp_2", [(1, 0)])
    return jnp.where(core == 1, own, back)


def shards(ways, decay_rate, drive_in, gate_in, norm_gain):
    total = decay_rate.shape[1] * lax.axis_size(SP)
    parts = lax.axis_size("tp")
    width = decay_rate.shape[2] * parts
    depth, term, pair = summarize(decay_rate, drive_in, total)
    factor, sums = localize(depth, term, gate_in)
    enter = entering_state(pair, ways)
    gated, power = gate_and_square(factor, sums, enter)
    powers = [power] + [
        lax.ppermute(power, "tp", [(i, (i + k) % parts) for i in range(parts)]) for k in (2, 1, 3)
    ]
    return scale(gated, powers, norm_gain, width)


def solution(mesh):
    torus = Mesh(mesh.devices.reshape(8, 4, 2, mesh.shape["tp"]), ("sp_0", "sp_1", "sp_2", "tp"))
    in_specs = (P(None, SP, "tp"), P(None, SP, "tp"), P(None, SP, "tp"), P("tp"))
    out_specs = P(None, SP, "tp")
    return jax.shard_map(
        functools.partial(shards, (8, 4)), mesh=torus, in_specs=in_specs, out_specs=out_specs, check_vma=False
    )
```

```python
import functools
import math

import jax
import jax.numpy as jnp
from jax import lax
from jax.experimental import pallas as pl
from jax.experimental.pallas import tpu as pltpu
from jax.sharding import Mesh
from jax.sharding import PartitionSpec as P

SP = ("sp_0", "sp_1", "sp_2")
CHIPS = ("sp_0", "sp_1")
BLOCK = 128
PIECE = 256
MIB = 1 << 20
VMEM = pl.BlockSpec(memory_space=pltpu.VMEM)
HBM = pl.BlockSpec(memory_space=pltpu.HBM)
SMEM = pl.BlockSpec(memory_space=pltpu.SMEM)


def stacked_triangle():
    row = lax.broadcasted_iota(jnp.int32, (BLOCK, 2 * BLOCK), 0)
    col = lax.broadcasted_iota(jnp.int32, (BLOCK, 2 * BLOCK), 1)
    return (row >= col % BLOCK).astype(jnp.bfloat16)


def running_sum(tri, x):
    high = x.astype(jnp.bfloat16)
    low = (x - high.astype(jnp.float32)).astype(jnp.bfloat16)
    return jnp.dot(tri, jnp.concatenate([high, low], axis=0), preferred_element_type=jnp.float32)


def piece_copy(hbm, vmem, sems, b, i):
    at = pl.ds(pl.multiple_of(i * PIECE, PIECE), PIECE)
    return pltpu.make_async_copy(hbm.at[b, at, :], vmem.at[b, at, :], sems.at[b * (hbm.shape[1] // PIECE) + i])


def start_all(sets):
    batch, length, _ = sets[0][0].shape
    for b in range(batch):
        for i in range(length // PIECE):
            for one in sets:
                piece_copy(*one, b, i).start()


def wait_at(sets, b, row):
    if row % PIECE == 0:
        for one in sets:
            piece_copy(*one, b, row // PIECE).wait()


def summary_kernel(total, rate_hbm, drive_hbm, out_ref, rate, drive, tri_ref, rate_sem, drive_sem):
    batch, length, channels = rate.shape
    sets = ((rate_hbm, rate, rate_sem), (drive_hbm, drive, drive_sem))
    start_all(sets)
    tri_ref[...] = stacked_triangle()
    to_log2 = math.log2(math.e) / total

    def one_batch(b, _):
        tri = tri_ref[...]
        lost = jnp.zeros((1, channels), jnp.float32)
        sums = jnp.zeros((8, channels), jnp.float32)
        for row in range(0, length, BLOCK):
            at = pl.ds(row, BLOCK)
            wait_at(sets, b, row)
            log_lost = running_sum(tri, rate[b, at, :]) * to_log2 + lost
            lost = log_lost[BLOCK - 1 :, :]
            term = jnp.exp2(log_lost) * drive[b, at, :].astype(jnp.float32)
            sums = sums + jnp.sum(term.reshape(BLOCK // 8, 8, channels), axis=0)
        out_ref[b, 0:1, :] = -lost
        out_ref[b, 1:2, :] = jnp.sum(sums, axis=0, keepdims=True)
        return 0

    lax.fori_loop(0, batch, one_batch, 0)


def summarize(decay_rate, drive_in, total):
    batch, length, channels = decay_rate.shape
    sems = pltpu.SemaphoreType.DMA((batch * length // PIECE,))
    return pl.pallas_call(
        functools.partial(summary_kernel, total),
        out_shape=jax.ShapeDtypeStruct((batch, 2, channels), jnp.float32),
        in_specs=[HBM] * 2,
        out_specs=VMEM,
        scratch_shapes=[
            pltpu.VMEM(decay_rate.shape, jnp.float32),
            pltpu.VMEM(drive_in.shape, jnp.bfloat16),
            pltpu.VMEM((BLOCK, 2 * BLOCK), jnp.bfloat16),
            sems,
            sems,
        ],
        compiler_params=pltpu.CompilerParams(vmem_limit_bytes=62 * MIB),
        cost_estimate=pl.CostEstimate(flops=1_000_000_000, bytes_accessed=6 * MIB, transcendentals=MIB),
        name="summarize",
    )(decay_rate, drive_in)


def local_kernel(
    total, rate_hbm, drive_hbm, gate_hbm, factor_ref, sum_ref, rate, drive, gate, tri_ref, rate_sem, drive_sem, gate_sem
):
    batch, length, channels = rate.shape
    sets = ((rate_hbm, rate, rate_sem), (drive_hbm, drive, drive_sem), (gate_hbm, gate, gate_sem))
    start_all(sets)
    tri_ref[...] = stacked_triangle()
    to_log2 = -math.log2(math.e) / total
    half = 0.5 * total**-0.5

    def one_batch(b, _):
        log_in = jnp.zeros((1, channels), jnp.float32)
        sum_in = jnp.zeros((1, channels), jnp.float32)
        tri = tri_ref[...]
        for row in range(0, length, BLOCK):
            at = pl.ds(row, BLOCK)
            wait_at(sets, b, row)
            log_kept = running_sum(tri, rate[b, at, :]) * to_log2 + log_in
            log_in = log_kept[BLOCK - 1 :, :]
            term = jnp.exp2(-log_kept) * drive[b, at, :].astype(jnp.float32)
            opened = half * jnp.tanh((0.5 * gate[b, at, :]).astype(jnp.float32)) + half
            factor_ref[b, at, :] = jnp.exp2(log_kept) * opened
            sums = running_sum(tri, term) + sum_in
            sum_in = sums[BLOCK - 1 :, :]
            sum_ref[b, at, :] = sums
        return 0

    lax.fori_loop(0, batch, one_batch, 0)


def localize(decay_rate, drive_in, gate_in, total):
    batch, length, channels = decay_rate.shape
    big = jax.ShapeDtypeStruct(decay_rate.shape, jnp.float32)
    sems = pltpu.SemaphoreType.DMA((batch * length // PIECE,))
    return pl.pallas_call(
        functools.partial(local_kernel, total),
        out_shape=(big, big),
        in_specs=[HBM] * 3,
        out_specs=(VMEM,) * 2,
        scratch_shapes=[
            pltpu.VMEM(decay_rate.shape, jnp.float32),
            pltpu.VMEM(drive_in.shape, jnp.bfloat16),
            pltpu.VMEM(gate_in.shape, jnp.bfloat16),
            pltpu.VMEM((BLOCK, 2 * BLOCK), jnp.bfloat16),
            sems,
            sems,
            sems,
        ],
        compiler_params=pltpu.CompilerParams(vmem_limit_bytes=20 * MIB),
        cost_estimate=pl.CostEstimate(flops=4_000_000_000, bytes_accessed=8 * MIB, transcendentals=3 * MIB),
        name="localize",
    )(decay_rate, drive_in, gate_in)


def enter_kernel(place_ref, all_ref, first_ref, out_ref):
    chips, pairs, _, channels = all_ref.shape
    place = place_ref[0]
    for p in range(pairs):
        state = jnp.zeros((1, channels), jnp.float32)
        for j in range(chips):
            kept = jnp.exp2(jnp.where(j < place, all_ref[j, p, 0:1, :], 0.0))
            state = kept * (state + jnp.where(j < place, all_ref[j, p, 1:2, :], 0.0))
        out_ref[0, p : p + 1, :] = state
        out_ref[1, p : p + 1, :] = jnp.exp2(first_ref[p, 0:1, :]) * (state + first_ref[p, 1:2, :])


def entering(place, everyone, first):
    chips, pairs, _, channels = everyone.shape
    return pl.pallas_call(
        enter_kernel,
        out_shape=jax.ShapeDtypeStruct((2, pairs, channels), jnp.float32),
        in_specs=[SMEM, VMEM, VMEM],
        out_specs=VMEM,
        compiler_params=pltpu.CompilerParams(vmem_limit_bytes=2 * MIB),
        name="entering",
    )(place, everyone, first)


def gate_kernel(factor_ref, sum_ref, enter_ref, gated_ref, power_ref):
    batch, length, channels = factor_ref.shape
    lane = lax.broadcasted_iota(jnp.int32, (8, 128), 1)

    def one_batch(b, _):
        enter = jnp.broadcast_to(enter_ref[pl.ds(b, 1), :], (8, channels))
        power = jnp.zeros((8, length // 8), jnp.float32)
        for j in range(length // 8):
            at = pl.ds(8 * j, 8)
            gated = factor_ref[b, at, :] * (sum_ref[b, at, :] + enter)
            gated_ref[b, at, :] = gated
            power = jnp.where(lane == j, jnp.sum(gated * gated, axis=-1, keepdims=True), power)
        power_ref[b] = power
        return 0

    lax.fori_loop(0, batch, one_batch, 0)


def gate_and_square(factor, sums, enter):
    batch, length, channels = factor.shape
    return pl.pallas_call(
        gate_kernel,
        out_shape=(
            jax.ShapeDtypeStruct(factor.shape, jnp.float32),
            jax.ShapeDtypeStruct((batch, 8, length // 8), jnp.float32),
        ),
        in_specs=[VMEM] * 3,
        out_specs=(VMEM, VMEM),
        compiler_params=pltpu.CompilerParams(vmem_limit_bytes=14 * MIB),
        cost_estimate=pl.CostEstimate(flops=8_000_000, bytes_accessed=12 * MIB, transcendentals=0),
        name="gate_and_square",
    )(factor, sums, enter)


def scale_kernel(width, gated_ref, p0_ref, p1_ref, p2_ref, p3_ref, gain_ref, out_hbm, out, sem):
    batch, length, channels = gated_ref.shape

    def copy(b):
        return pltpu.make_async_copy(out.at[b], out_hbm.at[b], sem.at[b])

    def one_batch(b, _):
        gain = jnp.broadcast_to(gain_ref[...], (8, channels))
        power = (p0_ref[b] + p1_ref[b]) + (p2_ref[b] + p3_ref[b])
        scale = lax.rsqrt(power * (1.0 / width) + 1e-06)
        for j in range(length // 16):
            parts = []
            for k in range(2):
                column = jnp.full((8, 128), 2 * j + k, jnp.int32)
                rows = jnp.take_along_axis(scale, column, axis=1)
                rows = jnp.concatenate([rows] * (channels // 128), axis=1)
                parts.append(gated_ref[b, pl.ds(16 * j + 8 * k, 8), :] * rows * gain)
            out[b, pl.ds(16 * j, 16), :] = jnp.concatenate(parts, axis=0).astype(jnp.bfloat16)
        copy(b).start()
        return 0

    lax.fori_loop(0, batch, one_batch, 0)
    for b in range(batch):
        copy(b).wait()


def scale(gated, powers, gain, width):
    batch, length, channels = gated.shape
    return pl.pallas_call(
        functools.partial(scale_kernel, width),
        out_shape=jax.ShapeDtypeStruct(gated.shape, jnp.bfloat16),
        in_specs=[VMEM] * 6,
        out_specs=HBM,
        scratch_shapes=[pltpu.VMEM(gated.shape, jnp.bfloat16), pltpu.SemaphoreType.DMA((batch,))],
        compiler_params=pltpu.CompilerParams(vmem_limit_bytes=8 * MIB),
        cost_estimate=pl.CostEstimate(flops=8_000_000, bytes_accessed=6 * MIB, transcendentals=0),
        name="scale",
    )(gated, *powers, gain.reshape(1, channels))


def join(earlier, later):
    return jnp.stack([earlier[:, 0] + later[:, 0], earlier[:, 1] + jnp.exp2(-earlier[:, 0]) * later[:, 1]], axis=1)


def entering_state(pair):
    half = pair.shape[0] // 2
    first_core = lax.axis_index("sp_2") == 0
    low, high = pair[:half], pair[half:]
    swap = [(0, 1), (1, 0)]
    got = lax.ppermute(jnp.where(first_core, high, low), "sp_2", swap)
    first = jnp.where(first_core, low, got)
    second = jnp.where(first_core, got, high)
    chip = join(first, second)
    chips = lax.axis_size(CHIPS)
    everyone = lax.all_to_all(jnp.broadcast_to(chip, (chips,) + chip.shape), CHIPS, 0, 0)
    both = entering(lax.axis_index(CHIPS).reshape(1), everyone, first)
    back = lax.ppermute(jnp.where(first_core, both[1], both[0]), "sp_2", swap)
    return jnp.where(
        first_core, jnp.concatenate([both[0], back], axis=0), jnp.concatenate([back, both[1]], axis=0)
    )


def shards(decay_rate, drive_in, gate_in, norm_gain):
    total = decay_rate.shape[1] * lax.axis_size(SP)
    parts = lax.axis_size("tp")
    width = decay_rate.shape[2] * parts
    enter = entering_state(summarize(decay_rate, drive_in, total))
    factor, sums = localize(decay_rate, drive_in, gate_in, total)
    gated, power = gate_and_square(factor, sums, enter)
    powers = [power] + [lax.ppermute(power, "tp", [(i, i ^ k) for i in range(parts)]) for k in (2, 1, 3)]
    return scale(gated, powers, norm_gain, width)


def solution(mesh):
    torus = Mesh(mesh.devices.reshape(8, 4, 2, mesh.shape["tp"]), ("sp_0", "sp_1", "sp_2", "tp"))
    in_specs = (P(None, SP, "tp"), P(None, SP, "tp"), P(None, SP, "tp"), P("tp"))
    out_specs = P(None, SP, "tp")
    return jax.shard_map(shards, mesh=torus, in_specs=in_specs, out_specs=out_specs, check_vma=False)
```

```python
import functools
import math

import jax
import jax.numpy as jnp
from jax import lax
from jax.experimental import pallas as pl
from jax.experimental.pallas import tpu as pltpu
from jax.sharding import Mesh
from jax.sharding import PartitionSpec as P

SP = ("sp_0", "sp_1", "sp_2")
CHIPS = ("sp_0", "sp_1")
BLOCK = 128
MIB = 1 << 20
VMEM = pl.BlockSpec(memory_space=pltpu.VMEM)
HBM = pl.BlockSpec(memory_space=pltpu.HBM)


def running_sum(tri, high, low):
    return jnp.dot(tri, jnp.concatenate([high, low], axis=0), preferred_element_type=jnp.float32)


def local_kernel(
    total, rate_hbm, drive_hbm, gate_hbm, factor_ref, sum_ref, mine_ref, other_ref, rate, drive, gate, pair, tri_ref, rate_sem, drive_sem, gate_sem
):
    batch, length, channels = rate.shape
    sets = ((rate_hbm, rate, rate_sem), (drive_hbm, drive, drive_sem), (gate_hbm, gate, gate_sem))

    def copies(b):
        return [pltpu.make_async_copy(hbm.at[b], vmem.at[b], sems.at[b]) for hbm, vmem, sems in sets]

    for b in range(batch):
        for copy in copies(b):
            copy.start()
    row = lax.broadcasted_iota(jnp.int32, (BLOCK, 2 * BLOCK), 0)
    col = lax.broadcasted_iota(jnp.int32, (BLOCK, 2 * BLOCK), 1)
    tri_ref[...] = (row >= col % BLOCK).astype(jnp.bfloat16)
    to_log2 = math.log2(math.e) / total
    middle = 0.5 * total**-0.5

    def one_batch(b, _):
        for copy in copies(b):
            copy.wait()
        tri = tri_ref[...]
        lost_in = jnp.zeros((1, channels), jnp.float32)
        sum_in = jnp.zeros((1, channels), jnp.float32)
        for first in range(0, length, BLOCK):
            at = pl.ds(first, BLOCK)
            rates = rate[b, at, :]
            high = rates.astype(jnp.bfloat16)
            low = (rates - high.astype(jnp.float32)).astype(jnp.bfloat16)
            lost = running_sum(tri, high, low) * to_log2 + lost_in
            lost_in = lost[BLOCK - 1 :, :]
            opened = middle * jnp.tanh((0.5 * gate[b, at, :]).astype(jnp.float32)) + middle
            factor_ref[b, at, :] = jnp.exp2(-lost) * opened
            drives = drive[b, at, :]
            grown = ((jnp.exp2(lost) - 1.0) * drives.astype(jnp.float32)).astype(jnp.bfloat16)
            sums = running_sum(tri, drives, grown) + sum_in
            sum_in = sums[BLOCK - 1 :, :]
            sum_ref[b, at, :] = sums
        pair[b, 0:1, :] = -lost_in
        pair[b, 1:2, :] = sum_in
        return 0

    lax.fori_loop(0, batch, one_batch, 0)
    core, half = lax.axis_index("sp_2"), batch // 2
    mine_ref[...] = pair[pl.ds(core * half, half)]
    other_ref[...] = pair[pl.ds((1 - core) * half, half)]


def localize(decay_rate, drive_in, gate_in, total):
    batch, length, channels = decay_rate.shape
    big = jax.ShapeDtypeStruct(decay_rate.shape, jnp.float32)
    pair = jax.ShapeDtypeStruct((batch // 2, 2, channels), jnp.float32)
    sems = pltpu.SemaphoreType.DMA((batch,))
    return pl.pallas_call(
        functools.partial(local_kernel, total),
        out_shape=(big, big, pair, pair),
        in_specs=[HBM] * 3,
        out_specs=(VMEM,) * 4,
        scratch_shapes=[
            pltpu.VMEM(decay_rate.shape, jnp.float32),
            pltpu.VMEM(drive_in.shape, jnp.bfloat16),
            pltpu.VMEM(gate_in.shape, jnp.bfloat16),
            pltpu.VMEM((batch, 2, channels), jnp.float32),
            pltpu.VMEM((BLOCK, 2 * BLOCK), jnp.bfloat16),
            sems,
            sems,
            sems,
        ],
        compiler_params=pltpu.CompilerParams(vmem_limit_bytes=20 * MIB),
        cost_estimate=pl.CostEstimate(flops=2_000_000_000, bytes_accessed=8 * MIB, transcendentals=3 * MIB),
        name="localize",
    )(decay_rate, drive_in, gate_in)


def meet_kernel(mine_ref, got_ref, first_ref, every_ref):
    first_core = lax.axis_index("sp_2") == 0
    for p in range(mine_ref.shape[0]):
        mine, got = mine_ref[p], got_ref[p]
        first = jnp.where(first_core, mine, got)
        second = jnp.where(first_core, got, mine)
        first_ref[p] = first
        kept = first[0:1] + second[0:1]
        sums = first[1:2] + jnp.exp2(-first[0:1]) * second[1:2]
        for j in range(every_ref.shape[0]):
            every_ref[j, p, 0:1, :] = kept
            every_ref[j, p, 1:2, :] = sums


def meet(mine, got, chips):
    return pl.pallas_call(
        meet_kernel,
        out_shape=(
            jax.ShapeDtypeStruct(mine.shape, jnp.float32),
            jax.ShapeDtypeStruct((chips,) + mine.shape, jnp.float32),
        ),
        in_specs=[VMEM] * 2,
        out_specs=(VMEM,) * 2,
        compiler_params=pltpu.CompilerParams(vmem_limit_bytes=2 * MIB),
        name="meet",
    )(mine, got)


def enter_kernel(every_ref, first_ref, mine_ref, other_ref):
    chips, pairs, _, channels = every_ref.shape
    place = lax.axis_index(CHIPS)
    first_core = lax.axis_index("sp_2") == 0
    for p in range(pairs):
        state = jnp.zeros((1, channels), jnp.float32)
        for j in range(chips):
            kept = jnp.exp2(jnp.where(j < place, every_ref[j, p, 0:1, :], 0.0))
            state = kept * (state + jnp.where(j < place, every_ref[j, p, 1:2, :], 0.0))
        after = jnp.exp2(first_ref[p, 0:1, :]) * (state + first_ref[p, 1:2, :])
        mine_ref[p : p + 1, :] = jnp.where(first_core, state, after)
        other_ref[p : p + 1, :] = jnp.where(first_core, after, state)


def entering(every, first):
    chips, pairs, _, channels = every.shape
    out = jax.ShapeDtypeStruct((pairs, channels), jnp.float32)
    return pl.pallas_call(
        enter_kernel,
        out_shape=(out, out),
        in_specs=[VMEM] * 2,
        out_specs=(VMEM,) * 2,
        compiler_params=pltpu.CompilerParams(vmem_limit_bytes=2 * MIB),
        name="entering",
    )(every, first)


def gate_kernel(factor_ref, sum_ref, mine_ref, got_ref, gated_ref, power_ref):
    batch, length, channels = factor_ref.shape
    lane = lax.broadcasted_iota(jnp.int32, (8, 128), 1)
    core, half = lax.axis_index("sp_2"), batch // 2

    def one_batch(b, _):
        mine, got = mine_ref[pl.ds(b % half, 1), :], got_ref[pl.ds(b % half, 1), :]
        enter = jnp.broadcast_to(jnp.where(b // half == core, mine, got), (8, channels))
        power = jnp.zeros((8, length // 8), jnp.float32)
        for j in range(length // 8):
            at = pl.ds(8 * j, 8)
            gated = factor_ref[b, at, :] * (sum_ref[b, at, :] + enter)
            gated_ref[b, at, :] = gated
            power = jnp.where(lane == j, jnp.sum(gated * gated, axis=-1, keepdims=True), power)
        power_ref[b] = power
        return 0

    lax.fori_loop(0, batch, one_batch, 0)


def gate_and_square(factor, sums, mine, got):
    batch, length, channels = factor.shape
    return pl.pallas_call(
        gate_kernel,
        out_shape=(
            jax.ShapeDtypeStruct(factor.shape, jnp.float32),
            jax.ShapeDtypeStruct((batch, 8, length // 8), jnp.float32),
        ),
        in_specs=[VMEM] * 4,
        out_specs=(VMEM, VMEM),
        compiler_params=pltpu.CompilerParams(vmem_limit_bytes=14 * MIB),
        cost_estimate=pl.CostEstimate(flops=8_000_000, bytes_accessed=12 * MIB, transcendentals=0),
        name="gate_and_square",
    )(factor, sums, mine, got)


def scale_kernel(width, gated_ref, p0_ref, p1_ref, p2_ref, p3_ref, gain_ref, out_hbm, out, sem):
    batch, length, channels = gated_ref.shape

    def copy(b):
        return pltpu.make_async_copy(out.at[b], out_hbm.at[b], sem.at[b])

    def one_batch(b, _):
        gain = jnp.broadcast_to(gain_ref[...], (8, channels))
        power = (p0_ref[b] + p1_ref[b]) + (p2_ref[b] + p3_ref[b])
        scale = lax.rsqrt(power * (1.0 / width) + 1e-06)
        for j in range(length // 16):
            parts = []
            for k in range(2):
                column = jnp.full((8, 128), 2 * j + k, jnp.int32)
                rows = jnp.take_along_axis(scale, column, axis=1)
                rows = jnp.concatenate([rows] * (channels // 128), axis=1)
                parts.append(gated_ref[b, pl.ds(16 * j + 8 * k, 8), :] * rows * gain)
            out[b, pl.ds(16 * j, 16), :] = jnp.concatenate(parts, axis=0).astype(jnp.bfloat16)
        copy(b).start()
        return 0

    lax.fori_loop(0, batch, one_batch, 0)
    for b in range(batch):
        copy(b).wait()


def scale(gated, powers, gain, width):
    batch, length, channels = gated.shape
    return pl.pallas_call(
        functools.partial(scale_kernel, width),
        out_shape=jax.ShapeDtypeStruct(gated.shape, jnp.bfloat16),
        in_specs=[VMEM] * 6,
        out_specs=HBM,
        scratch_shapes=[pltpu.VMEM(gated.shape, jnp.bfloat16), pltpu.SemaphoreType.DMA((batch,))],
        compiler_params=pltpu.CompilerParams(vmem_limit_bytes=8 * MIB),
        cost_estimate=pl.CostEstimate(flops=8_000_000, bytes_accessed=6 * MIB, transcendentals=0),
        name="scale",
    )(gated, *powers, gain.reshape(1, channels))


def shards(decay_rate, drive_in, gate_in, norm_gain):
    total = decay_rate.shape[1] * lax.axis_size(SP)
    parts = lax.axis_size("tp")
    width = decay_rate.shape[2] * parts
    swap = [(0, 1), (1, 0)]
    decay_rate, drive_in, gate_in = (
        pltpu.with_memory_space_constraint(array, pltpu.HBM) for array in (decay_rate, drive_in, gate_in)
    )
    factor, sums, mine, other = localize(decay_rate, drive_in, gate_in, total)
    first, every = meet(mine, lax.ppermute(other, "sp_2", swap), lax.axis_size(CHIPS))
    every = lax.all_to_all(every, CHIPS, 0, 0)
    every, norm_gain = lax.optimization_barrier((every, norm_gain))
    mine, other = entering(every, first)
    gated, power = gate_and_square(factor, sums, mine, lax.ppermute(other, "sp_2", swap))
    powers = [power] + [lax.ppermute(power, "tp", [(i, i ^ k) for i in range(parts)]) for k in (2, 1, 3)]
    return scale(gated, powers, norm_gain, width)


def solution(mesh):
    torus = Mesh(mesh.devices.reshape(8, 4, 2, mesh.shape["tp"]), ("sp_0", "sp_1", "sp_2", "tp"))
    in_specs = (P(None, SP, "tp"), P(None, SP, "tp"), P(None, SP, "tp"), P("tp"))
    out_specs = P(None, SP, "tp")
    return jax.shard_map(shards, mesh=torus, in_specs=in_specs, out_specs=out_specs, check_vma=False)
```

```python
import functools
import math

import jax
import jax.numpy as jnp
from jax import lax
from jax.experimental import pallas as pl
from jax.experimental.pallas import tpu as pltpu
from jax.sharding import Mesh
from jax.sharding import PartitionSpec as P

SP = ("sp_0", "sp_1", "sp_2")
CHIPS = ("sp_0", "sp_1")
BLOCK = 128
MIB = 1 << 20
VMEM = pl.BlockSpec(memory_space=pltpu.VMEM)
HBM = pl.BlockSpec(memory_space=pltpu.HBM)


def local_kernel(
    total,
    rate_hbm,
    drive_hbm,
    gate_hbm,
    factor_ref,
    sum_ref,
    lost_ref,
    carry_ref,
    mine_ref,
    other_ref,
    rate,
    drive,
    gate,
    pair,
    tri_ref,
    rate_sem,
    drive_sem,
    gate_sem,
):
    batch, length, channels = rate.shape
    sets = ((rate_hbm, rate, rate_sem), (drive_hbm, drive, drive_sem), (gate_hbm, gate, gate_sem))

    def copies(b):
        return [pltpu.make_async_copy(hbm.at[b], vmem.at[b], sems.at[b]) for hbm, vmem, sems in sets]

    for b in range(batch):
        for copy in copies(b):
            copy.start()
    row = lax.broadcasted_iota(jnp.int32, (BLOCK, 2 * BLOCK), 0)
    col = lax.broadcasted_iota(jnp.int32, (BLOCK, 2 * BLOCK), 1)
    tri_ref[...] = (row >= col % BLOCK).astype(jnp.bfloat16)
    to_log2 = math.log2(math.e) / total

    def one_batch(b, _):
        for copy in copies(b):
            copy.wait()
        lost_in = jnp.zeros((1, channels), jnp.float32)
        carry = jnp.zeros((1, channels), jnp.float32)
        for k in range(length // BLOCK):
            at = pl.ds(k * BLOCK, BLOCK)
            rates = rate[b, at, :]
            lost = to_log2 * jnp.dot(
                tri_ref[:, :BLOCK], rates.astype(jnp.bfloat16), preferred_element_type=jnp.float32
            )
            opened = jnp.tanh((0.5 * gate[b, at, :]).astype(jnp.float32)) + 1.0
            factor_ref[b, at, :] = jnp.exp2(-lost) * opened
            drives = drive[b, at, :]
            grown = (jnp.exp2(lost) - 1.0).astype(jnp.bfloat16) * drives
            sums = jnp.dot(
                tri_ref[...], jnp.concatenate([drives, grown], axis=0), preferred_element_type=jnp.float32
            )
            sum_ref[b, at, :] = sums
            lost_ref[b, k : k + 1, :] = lost_in
            carry_ref[b, k : k + 1, :] = carry
            carry = carry + jnp.exp2(lost_in) * sums[BLOCK - 1 :, :]
            whole = jnp.sum(rates.reshape(BLOCK // 8, 8, channels), axis=0)
            lost_in = lost_in + to_log2 * jnp.sum(whole, axis=0, keepdims=True)
        pair[b, 0:1, :] = lost_in
        pair[b, 1:2, :] = carry
        return 0

    lax.fori_loop(0, batch, one_batch, 0)
    core, half = lax.axis_index("sp_2"), batch // 2
    mine_ref[...] = pair[pl.ds(core * half, half)]
    other_ref[...] = pair[pl.ds((1 - core) * half, half)]


def localize(decay_rate, drive_in, gate_in, total):
    batch, length, channels = decay_rate.shape
    big = jax.ShapeDtypeStruct(decay_rate.shape, jnp.float32)
    blocks = jax.ShapeDtypeStruct((batch, length // BLOCK, channels), jnp.float32)
    pair = jax.ShapeDtypeStruct((batch // 2, 2, channels), jnp.float32)
    sems = pltpu.SemaphoreType.DMA((batch,))
    return pl.pallas_call(
        functools.partial(local_kernel, total),
        out_shape=(big, big, blocks, blocks, pair, pair),
        in_specs=[HBM] * 3,
        out_specs=(VMEM,) * 6,
        scratch_shapes=[
            pltpu.VMEM(decay_rate.shape, jnp.float32),
            pltpu.VMEM(drive_in.shape, jnp.bfloat16),
            pltpu.VMEM(gate_in.shape, jnp.bfloat16),
            pltpu.VMEM((batch, 2, channels), jnp.float32),
            pltpu.VMEM((BLOCK, 2 * BLOCK), jnp.bfloat16),
            sems,
            sems,
            sems,
        ],
        compiler_params=pltpu.CompilerParams(vmem_limit_bytes=20 * MIB),
        cost_estimate=pl.CostEstimate(flops=2_000_000_000, bytes_accessed=8 * MIB, transcendentals=3 * MIB),
        name="localize",
    )(decay_rate, drive_in, gate_in)


def meet_kernel(mine_ref, got_ref, first_ref, every_ref):
    first_core = lax.axis_index("sp_2") == 0
    for p in range(mine_ref.shape[0]):
        mine, got = mine_ref[p], got_ref[p]
        first = jnp.where(first_core, mine, got)
        second = jnp.where(first_core, got, mine)
        first_ref[p] = first
        lost = first[0:1] + second[0:1]
        sums = first[1:2] + jnp.exp2(first[0:1]) * second[1:2]
        for j in range(every_ref.shape[0]):
            every_ref[j, p, 0:1, :] = lost
            every_ref[j, p, 1:2, :] = sums


def meet(mine, got, chips):
    return pl.pallas_call(
        meet_kernel,
        out_shape=(
            jax.ShapeDtypeStruct(mine.shape, jnp.float32),
            jax.ShapeDtypeStruct((chips,) + mine.shape, jnp.float32),
        ),
        in_specs=[VMEM] * 2,
        out_specs=(VMEM,) * 2,
        compiler_params=pltpu.CompilerParams(vmem_limit_bytes=2 * MIB),
        name="meet",
    )(mine, got)


def enter_kernel(every_ref, first_ref, mine_ref, other_ref):
    chips, pairs, _, channels = every_ref.shape
    place = lax.axis_index(CHIPS)
    first_core = lax.axis_index("sp_2") == 0
    for p in range(pairs):
        state = jnp.zeros((1, channels), jnp.float32)
        for j in range(chips):
            kept = jnp.exp2(-jnp.where(j < place, every_ref[j, p, 0:1, :], 0.0))
            state = kept * (state + jnp.where(j < place, every_ref[j, p, 1:2, :], 0.0))
        after = jnp.exp2(-first_ref[p, 0:1, :]) * (state + first_ref[p, 1:2, :])
        mine_ref[p : p + 1, :] = jnp.where(first_core, state, after)
        other_ref[p : p + 1, :] = jnp.where(first_core, after, state)


def entering(every, first):
    chips, pairs, _, channels = every.shape
    out = jax.ShapeDtypeStruct((pairs, channels), jnp.float32)
    return pl.pallas_call(
        enter_kernel,
        out_shape=(out, out),
        in_specs=[VMEM] * 2,
        out_specs=(VMEM,) * 2,
        compiler_params=pltpu.CompilerParams(vmem_limit_bytes=2 * MIB),
        name="entering",
    )(every, first)


def gate_kernel(mine, factor_ref, sum_ref, lost_ref, carry_ref, enter_ref, gated_ref, power_ref):
    half, length, channels = gated_ref.shape
    lane = lax.broadcasted_iota(jnp.int32, (8, length // 8), 1)
    core = lax.axis_index("sp_2")
    start = half * (core if mine else 1 - core)

    def one_batch(p, _):
        b = start + p
        enter = jnp.exp2(-lost_ref[b]) * (enter_ref[pl.ds(p, 1), :] + carry_ref[b])
        power = jnp.zeros((8, length // 8), jnp.float32)
        for k in range(length // BLOCK):
            state = jnp.broadcast_to(enter[k : k + 1, :], (8, channels))
            for j in range(k * BLOCK // 8, (k + 1) * BLOCK // 8):
                at = pl.ds(8 * j, 8)
                gated = factor_ref[b, at, :] * (sum_ref[b, at, :] + state)
                gated_ref[p, at, :] = gated
                power = jnp.where(lane == j, jnp.sum(gated * gated, axis=-1, keepdims=True), power)
        power_ref[p] = power
        return 0

    lax.fori_loop(0, half, one_batch, 0)


def gate_and_square(mine, local, enter, name):
    batch, length, channels = local[0].shape
    half = batch // 2
    return pl.pallas_call(
        functools.partial(gate_kernel, mine),
        out_shape=(
            jax.ShapeDtypeStruct((half, length, channels), jnp.float32),
            jax.ShapeDtypeStruct((half, 8, length // 8), jnp.float32),
        ),
        in_specs=[VMEM] * 5,
        out_specs=(VMEM, VMEM),
        compiler_params=pltpu.CompilerParams(vmem_limit_bytes=14 * MIB),
        cost_estimate=pl.CostEstimate(flops=4_000_000, bytes_accessed=6 * MIB, transcendentals=0),
        name=name,
    )(*local, enter)


def scale_kernel(middle, width, mine_ref, got_ref, p0_ref, p1_ref, p2_ref, p3_ref, gain_ref, out_hbm, out, sem):
    half, length, channels = mine_ref.shape
    core = lax.axis_index("sp_2")

    def copy(h, p):
        b = half * (core if h == 0 else 1 - core) + p
        return pltpu.make_async_copy(out.at[h, p], out_hbm.at[b], sem.at[h, p])

    def one_batch(p, _):
        gain = jnp.broadcast_to(gain_ref[...], (8, channels))
        for h, gated_ref in enumerate((mine_ref, got_ref)):
            power = (p0_ref[h, p] + p1_ref[h, p]) + (p2_ref[h, p] + p3_ref[h, p])
            scale = middle * lax.rsqrt(power * (middle * middle / width) + 1e-06)
            for j in range(length // 16):
                parts = []
                for k in range(2):
                    column = jnp.full((8, 128), 2 * j + k, jnp.int32)
                    rows = jnp.take_along_axis(scale, column, axis=1)
                    rows = jnp.concatenate([rows] * (channels // 128), axis=1)
                    parts.append(gated_ref[p, pl.ds(16 * j + 8 * k, 8), :] * rows * gain)
                out[h, p, pl.ds(16 * j, 16), :] = jnp.concatenate(parts, axis=0).astype(jnp.bfloat16)
            copy(h, p).start()
        return 0

    lax.fori_loop(0, half, one_batch, 0)
    for p in range(half):
        for h in range(2):
            copy(h, p).wait()


def scale(mine, got, powers, gain, middle, width):
    half, length, channels = mine.shape
    return pl.pallas_call(
        functools.partial(scale_kernel, middle, width),
        out_shape=jax.ShapeDtypeStruct((2 * half, length, channels), jnp.bfloat16),
        in_specs=[VMEM] * 7,
        out_specs=HBM,
        scratch_shapes=[pltpu.VMEM((2,) + mine.shape, jnp.bfloat16), pltpu.SemaphoreType.DMA((2, half))],
        compiler_params=pltpu.CompilerParams(vmem_limit_bytes=8 * MIB),
        cost_estimate=pl.CostEstimate(flops=8_000_000, bytes_accessed=6 * MIB, transcendentals=0),
        name="scale",
    )(mine, got, *powers, gain.reshape(1, channels))


def shards(decay_rate, drive_in, gate_in, norm_gain):
    total = decay_rate.shape[1] * lax.axis_size(SP)
    parts = lax.axis_size("tp")
    width = decay_rate.shape[2] * parts
    swap = [(0, 1), (1, 0)]
    decay_rate, drive_in, gate_in = (
        pltpu.with_memory_space_constraint(array, pltpu.HBM) for array in (decay_rate, drive_in, gate_in)
    )
    *local, mine, other = localize(decay_rate, drive_in, gate_in, total)
    first, every = meet(mine, lax.ppermute(other, "sp_2", swap), lax.axis_size(CHIPS))
    every = lax.all_to_all(every, CHIPS, 0, 0)
    every, norm_gain = lax.optimization_barrier((every, norm_gain))
    mine, other = entering(every, first)
    got = lax.ppermute(other, "sp_2", swap)
    gated_mine, power_mine = gate_and_square(True, local, mine, "gate_mine")
    gated_got, power_got = gate_and_square(False, local, got, "gate_got")
    power = jnp.stack([power_mine, power_got])
    powers = [power] + [lax.ppermute(power, "tp", [(i, i ^ k) for i in range(parts)]) for k in (1, 3, 2)]
    return scale(gated_mine, gated_got, powers, norm_gain, 0.5 * total**-0.5, width)


def solution(mesh):
    torus = Mesh(mesh.devices.reshape(8, 4, 2, mesh.shape["tp"]), ("sp_0", "sp_1", "sp_2", "tp"))
    in_specs = (P(None, SP, "tp"), P(None, SP, "tp"), P(None, SP, "tp"), P("tp"))
    out_specs = P(None, SP, "tp")
    return jax.shard_map(shards, mesh=torus, in_specs=in_specs, out_specs=out_specs, check_vma=False)
```

```python
import functools
import math

import jax
import jax.numpy as jnp
from jax import lax
from jax.experimental import pallas as pl
from jax.experimental.pallas import tpu as pltpu
from jax.sharding import Mesh
from jax.sharding import PartitionSpec as P

SP = ("sp_0", "sp_1", "sp_2")
CHIPS = ("sp_0", "sp_1")
BLOCK = 128
PIECE = 1024
MIB = 1 << 20
VMEM = pl.BlockSpec(memory_space=pltpu.VMEM)
HBM = pl.BlockSpec(memory_space=pltpu.HBM)


def local_kernel(
    total,
    rate_hbm,
    drive_hbm,
    gate_hbm,
    kept_ref,
    sum_ref,
    lost_ref,
    carry_ref,
    gate_ref,
    mine_ref,
    other_ref,
    rate,
    drive,
    pair,
    tri_ref,
    rate_sem,
    drive_sem,
    gate_sem,
):
    batch, length, channels = rate.shape
    sets = ((rate_hbm, rate, rate_sem), (drive_hbm, drive, drive_sem))
    pieces = length // PIECE

    def copies(b, i):
        at = pl.ds(pl.multiple_of(i * PIECE, PIECE), PIECE)
        return [
            pltpu.make_async_copy(hbm.at[b, at, :], vmem.at[b, at, :], sems.at[b * pieces + i]) for hbm, vmem, sems in sets
        ]

    for b in range(batch):
        for i in range(pieces):
            for copy in copies(b, i):
                copy.start()
    gates = [pltpu.make_async_copy(gate_hbm.at[b], gate_ref.at[b], gate_sem.at[b]) for b in range(batch)]
    for copy in gates:
        copy.start()
    row = lax.broadcasted_iota(jnp.int32, (BLOCK, 2 * BLOCK), 0)
    col = lax.broadcasted_iota(jnp.int32, (BLOCK, 2 * BLOCK), 1)
    tri_ref[...] = (row >= col % BLOCK).astype(jnp.bfloat16)
    to_log2 = math.log2(math.e) / total

    def one_piece(n, entered):
        b, i = n // pieces, n % pieces
        for copy in copies(b, i):
            copy.wait()
        lost_in, carry = (jnp.where(i == 0, 0.0, rows) for rows in entered)
        for k in range(PIECE // BLOCK):
            block = i * (PIECE // BLOCK) + k
            at = pl.ds(pl.multiple_of(block * BLOCK, BLOCK), BLOCK)
            rates = rate[b, at, :]
            lost = to_log2 * jnp.dot(
                tri_ref[:, :BLOCK], rates.astype(jnp.bfloat16), preferred_element_type=jnp.float32
            )
            kept_ref[b, at, :] = jnp.exp2(-lost)
            drives = drive[b, at, :]
            grown = (jnp.exp2(lost) - 1.0).astype(jnp.bfloat16) * drives
            sums = jnp.dot(
                tri_ref[...], jnp.concatenate([drives, grown], axis=0), preferred_element_type=jnp.float32
            )
            sum_ref[b, at, :] = sums
            lost_ref[b, pl.ds(block, 1), :] = lost_in
            carry_ref[b, pl.ds(block, 1), :] = carry
            carry = carry + jnp.exp2(lost_in) * sums[BLOCK - 1 :, :]
            whole = jnp.sum(rates.reshape(BLOCK // 8, 8, channels), axis=0)
            lost_in = lost_in + to_log2 * jnp.sum(whole, axis=0, keepdims=True)
        pair[b, 0:1, :] = lost_in
        pair[b, 1:2, :] = carry
        return lost_in, carry

    start = jnp.zeros((1, channels), jnp.float32)
    lax.fori_loop(0, batch * pieces, one_piece, (start, start))
    core, half = lax.axis_index("sp_2"), batch // 2
    mine_ref[...] = pair[pl.ds(core * half, half)]
    other_ref[...] = pair[pl.ds((1 - core) * half, half)]
    for copy in gates:
        copy.wait()


def localize(decay_rate, drive_in, gate_in, total):
    batch, length, channels = decay_rate.shape
    big = jax.ShapeDtypeStruct(decay_rate.shape, jnp.float32)
    blocks = jax.ShapeDtypeStruct((batch, length // BLOCK, channels), jnp.float32)
    pair = jax.ShapeDtypeStruct((batch // 2, 2, channels), jnp.float32)
    sems = pltpu.SemaphoreType.DMA((batch * length // PIECE,))
    return pl.pallas_call(
        functools.partial(local_kernel, total),
        out_shape=(big, big, blocks, blocks, jax.ShapeDtypeStruct(gate_in.shape, gate_in.dtype), pair, pair),
        in_specs=[HBM] * 3,
        out_specs=(VMEM,) * 7,
        scratch_shapes=[
            pltpu.VMEM(decay_rate.shape, jnp.float32),
            pltpu.VMEM(drive_in.shape, jnp.bfloat16),
            pltpu.VMEM((batch, 2, channels), jnp.float32),
            pltpu.VMEM((BLOCK, 2 * BLOCK), jnp.bfloat16),
            sems,
            sems,
            pltpu.SemaphoreType.DMA((batch,)),
        ],
        compiler_params=pltpu.CompilerParams(vmem_limit_bytes=20 * MIB),
        cost_estimate=pl.CostEstimate(flops=2_000_000_000, bytes_accessed=8 * MIB, transcendentals=2 * MIB),
        name="localize",
    )(decay_rate, drive_in, gate_in)


def open_kernel(kept_ref, gate_ref, factor_ref):
    batch, length, channels = kept_ref.shape

    def one_piece(n, _):
        at = pl.ds(pl.multiple_of(n * BLOCK, BLOCK), BLOCK)
        for b in range(batch):
            opened = jnp.tanh((0.5 * gate_ref[b, at, :]).astype(jnp.float32)) + 1.0
            factor_ref[b, at, :] = kept_ref[b, at, :] * opened
        return 0

    lax.fori_loop(0, length // BLOCK, one_piece, 0)


def open_gate(kept, gate):
    return pl.pallas_call(
        open_kernel,
        out_shape=jax.ShapeDtypeStruct(kept.shape, jnp.float32),
        in_specs=[VMEM] * 2,
        out_specs=VMEM,
        input_output_aliases={0: 0},
        compiler_params=pltpu.CompilerParams(vmem_limit_bytes=12 * MIB),
        cost_estimate=pl.CostEstimate(flops=8_000_000, bytes_accessed=10 * MIB, transcendentals=MIB),
        name="open_gate",
    )(kept, gate)


def meet_kernel(mine_ref, got_ref, first_ref, every_ref):
    first_core = lax.axis_index("sp_2") == 0
    for p in range(mine_ref.shape[0]):
        mine, got = mine_ref[p], got_ref[p]
        first = jnp.where(first_core, mine, got)
        second = jnp.where(first_core, got, mine)
        first_ref[p] = first
        lost = first[0:1] + second[0:1]
        sums = first[1:2] + jnp.exp2(first[0:1]) * second[1:2]
        for j in range(every_ref.shape[0]):
            every_ref[j, p, 0:1, :] = lost
            every_ref[j, p, 1:2, :] = sums


def meet(mine, got, chips):
    return pl.pallas_call(
        meet_kernel,
        out_shape=(
            jax.ShapeDtypeStruct(mine.shape, jnp.float32),
            jax.ShapeDtypeStruct((chips,) + mine.shape, jnp.float32),
        ),
        in_specs=[VMEM] * 2,
        out_specs=(VMEM,) * 2,
        compiler_params=pltpu.CompilerParams(vmem_limit_bytes=2 * MIB),
        name="meet",
    )(mine, got)


def enter_kernel(every_ref, first_ref, mine_ref, other_ref):
    chips, pairs, _, channels = every_ref.shape
    place = lax.axis_index(CHIPS)
    first_core = lax.axis_index("sp_2") == 0
    for p in range(pairs):
        state = jnp.zeros((1, channels), jnp.float32)
        for j in range(chips):
            kept = jnp.exp2(-jnp.where(j < place, every_ref[j, p, 0:1, :], 0.0))
            state = kept * (state + jnp.where(j < place, every_ref[j, p, 1:2, :], 0.0))
        after = jnp.exp2(-first_ref[p, 0:1, :]) * (state + first_ref[p, 1:2, :])
        mine_ref[p : p + 1, :] = jnp.where(first_core, state, after)
        other_ref[p : p + 1, :] = jnp.where(first_core, after, state)


def entering(every, first):
    chips, pairs, _, channels = every.shape
    out = jax.ShapeDtypeStruct((pairs, channels), jnp.float32)
    return pl.pallas_call(
        enter_kernel,
        out_shape=(out, out),
        in_specs=[VMEM] * 2,
        out_specs=(VMEM,) * 2,
        compiler_params=pltpu.CompilerParams(vmem_limit_bytes=2 * MIB),
        name="entering",
    )(every, first)


def gate_kernel(mine, factor_ref, sum_ref, lost_ref, carry_ref, enter_ref, gain_ref, gated_ref, power_ref):
    half, length, channels = gated_ref.shape
    lane = lax.broadcasted_iota(jnp.int32, (8, length // 8), 1)
    core = lax.axis_index("sp_2")
    start = half * (core if mine else 1 - core)

    def one_batch(p, _):
        b = start + p
        enter = jnp.exp2(-lost_ref[b]) * (enter_ref[pl.ds(p, 1), :] + carry_ref[b])
        gain = jnp.broadcast_to(gain_ref[...], (8, channels))
        power = jnp.zeros((8, length // 8), jnp.float32)
        for k in range(length // BLOCK):
            state = jnp.broadcast_to(enter[k : k + 1, :], (8, channels))
            for j in range(k * BLOCK // 8, (k + 1) * BLOCK // 8):
                at = pl.ds(8 * j, 8)
                gated = factor_ref[b, at, :] * (sum_ref[b, at, :] + state)
                gated_ref[p, at, :] = gated * gain
                power = jnp.where(lane == j, jnp.sum(gated * gated, axis=-1, keepdims=True), power)
        power_ref[p] = power
        return 0

    lax.fori_loop(0, half, one_batch, 0)


def gate_and_square(mine, local, enter, gain, name):
    batch, length, channels = local[0].shape
    half = batch // 2
    return pl.pallas_call(
        functools.partial(gate_kernel, mine),
        out_shape=(
            jax.ShapeDtypeStruct((half, length, channels), jnp.float32),
            jax.ShapeDtypeStruct((half, 8, length // 8), jnp.float32),
        ),
        in_specs=[VMEM] * 6,
        out_specs=(VMEM, VMEM),
        compiler_params=pltpu.CompilerParams(vmem_limit_bytes=14 * MIB),
        cost_estimate=pl.CostEstimate(flops=4_000_000, bytes_accessed=6 * MIB, transcendentals=0),
        name=name,
    )(*local, enter, gain)


def scale_kernel(middle, width, mine_ref, got_ref, p0_ref, p1_ref, p2_ref, p3_ref, out_hbm, out, sem):
    half, length, channels = mine_ref.shape
    core = lax.axis_index("sp_2")

    def copy(h, p):
        b = half * (core if h == 0 else 1 - core) + p
        return pltpu.make_async_copy(out.at[h, p], out_hbm.at[b], sem.at[h, p])

    def one_batch(p, _):
        for h, gated_ref in enumerate((mine_ref, got_ref)):
            power = (p0_ref[h, p] + p1_ref[h, p]) + (p2_ref[h, p] + p3_ref[h, p])
            scale = middle * lax.rsqrt(power * (middle * middle / width) + 1e-06)
            for j in range(length // 16):
                parts = []
                for k in range(2):
                    column = jnp.full((8, 128), 2 * j + k, jnp.int32)
                    rows = jnp.take_along_axis(scale, column, axis=1)
                    rows = jnp.concatenate([rows] * (channels // 128), axis=1)
                    parts.append(gated_ref[p, pl.ds(16 * j + 8 * k, 8), :] * rows)
                out[h, p, pl.ds(16 * j, 16), :] = jnp.concatenate(parts, axis=0).astype(jnp.bfloat16)
            copy(h, p).start()
        return 0

    lax.fori_loop(0, half, one_batch, 0)
    for p in range(half):
        for h in range(2):
            copy(h, p).wait()


def scale(mine, got, powers, middle, width):
    half, length, channels = mine.shape
    return pl.pallas_call(
        functools.partial(scale_kernel, middle, width),
        out_shape=jax.ShapeDtypeStruct((2 * half, length, channels), jnp.bfloat16),
        in_specs=[VMEM] * 6,
        out_specs=HBM,
        scratch_shapes=[pltpu.VMEM((2,) + mine.shape, jnp.bfloat16), pltpu.SemaphoreType.DMA((2, half))],
        compiler_params=pltpu.CompilerParams(vmem_limit_bytes=8 * MIB),
        cost_estimate=pl.CostEstimate(flops=8_000_000, bytes_accessed=6 * MIB, transcendentals=0),
        name="scale",
    )(mine, got, *powers)


def shards(decay_rate, drive_in, gate_in, norm_gain):
    total = decay_rate.shape[1] * lax.axis_size(SP)
    parts = lax.axis_size("tp")
    width = decay_rate.shape[2] * parts
    swap = [(0, 1), (1, 0)]
    decay_rate, drive_in, gate_in = (
        pltpu.with_memory_space_constraint(array, pltpu.HBM) for array in (decay_rate, drive_in, gate_in)
    )
    kept, sums, lost, carry, gate, mine, other = localize(decay_rate, drive_in, gate_in, total)
    got = lax.ppermute(other, "sp_2", swap)
    factor = open_gate(kept, gate)
    got, factor = lax.optimization_barrier((got, factor))
    first, every = meet(mine, got, lax.axis_size(CHIPS))
    every = lax.all_to_all(every, CHIPS, 0, 0)
    every, factor, norm_gain = lax.optimization_barrier((every, factor, norm_gain))
    mine, other = entering(every, first)
    got = lax.ppermute(other, "sp_2", swap)
    local, gain = (factor, sums, lost, carry), norm_gain.reshape(1, -1)
    gated_mine, power_mine = gate_and_square(True, local, mine, gain, "gate_mine")
    gated_got, power_got = gate_and_square(False, local, got, gain, "gate_got")
    power = jnp.stack([power_mine, power_got])
    powers = [power] + [lax.ppermute(power, "tp", [(i, i ^ k) for i in range(parts)]) for k in (1, 3, 2)]
    return scale(gated_mine, gated_got, powers, 0.5 * total**-0.5, width)


def solution(mesh):
    torus = Mesh(mesh.devices.reshape(8, 4, 2, mesh.shape["tp"]), ("sp_0", "sp_1", "sp_2", "tp"))
    in_specs = (P(None, SP, "tp"), P(None, SP, "tp"), P(None, SP, "tp"), P("tp"))
    out_specs = P(None, SP, "tp")
    return jax.shard_map(shards, mesh=torus, in_specs=in_specs, out_specs=out_specs, check_vma=False)
```

```python
import functools
import math

import jax
import jax.numpy as jnp
from jax import lax
from jax.experimental import pallas as pl
from jax.experimental.pallas import tpu as pltpu
from jax.sharding import Mesh
from jax.sharding import PartitionSpec as P

SP = ("sp_0", "sp_1", "sp_2")
CHIPS = ("sp_0", "sp_1")
BLOCK = 128
PIECE = 1024
LEAVING = 256
MIB = 1 << 20
VMEM = pl.BlockSpec(memory_space=pltpu.VMEM)
HBM = pl.BlockSpec(memory_space=pltpu.HBM)


def local_kernel(
    total,
    rate_hbm,
    drive_hbm,
    gate_hbm,
    kept_ref,
    sum_ref,
    lost_ref,
    carry_ref,
    gate_ref,
    mine_ref,
    other_ref,
    rate,
    drive,
    pair,
    tri_ref,
    rate_sem,
    drive_sem,
    gate_sem,
):
    batch, length, channels = rate.shape
    sets = ((rate_hbm, rate, rate_sem), (drive_hbm, drive, drive_sem))
    pieces = length // PIECE

    def copies(b, i):
        at = pl.ds(pl.multiple_of(i * PIECE, PIECE), PIECE)
        return [
            pltpu.make_async_copy(hbm.at[b, at, :], vmem.at[b, at, :], sems.at[b * pieces + i]) for hbm, vmem, sems in sets
        ]

    for b in range(batch):
        for i in range(pieces):
            for copy in copies(b, i):
                copy.start()
    gates = [pltpu.make_async_copy(gate_hbm.at[b], gate_ref.at[b], gate_sem.at[b]) for b in range(batch)]
    for copy in gates:
        copy.start()
    row = lax.broadcasted_iota(jnp.int32, (BLOCK, 2 * BLOCK), 0)
    col = lax.broadcasted_iota(jnp.int32, (BLOCK, 2 * BLOCK), 1)
    tri_ref[...] = (row >= col % BLOCK).astype(jnp.bfloat16)
    to_log2 = math.log2(math.e) / total

    def one_piece(n, entered):
        b, i = n // pieces, n % pieces
        for copy in copies(b, i):
            copy.wait()
        lost_in, carry = (jnp.where(i == 0, 0.0, rows) for rows in entered)
        for k in range(PIECE // BLOCK):
            block = i * (PIECE // BLOCK) + k
            at = pl.ds(pl.multiple_of(block * BLOCK, BLOCK), BLOCK)
            rates = rate[b, at, :]
            lost = to_log2 * jnp.dot(
                tri_ref[:, :BLOCK], rates.astype(jnp.bfloat16), preferred_element_type=jnp.float32
            )
            kept_ref[b, at, :] = jnp.exp2(-lost)
            drives = drive[b, at, :]
            grown = (jnp.exp2(lost) - 1.0).astype(jnp.bfloat16) * drives
            sums = jnp.dot(
                tri_ref[...], jnp.concatenate([drives, grown], axis=0), preferred_element_type=jnp.float32
            )
            sum_ref[b, at, :] = sums
            lost_ref[b, pl.ds(block, 1), :] = lost_in
            carry_ref[b, pl.ds(block, 1), :] = carry
            carry = carry + jnp.exp2(lost_in) * sums[BLOCK - 1 :, :]
            whole = jnp.sum(rates.reshape(BLOCK // 8, 8, channels), axis=0)
            lost_in = lost_in + to_log2 * jnp.sum(whole, axis=0, keepdims=True)
        pair[b, 0:1, :] = lost_in
        pair[b, 1:2, :] = carry
        return lost_in, carry

    start = jnp.zeros((1, channels), jnp.float32)
    lax.fori_loop(0, batch * pieces, one_piece, (start, start))
    core, half = lax.axis_index("sp_2"), batch // 2
    mine_ref[...] = pair[pl.ds(core * half, half)]
    other_ref[...] = pair[pl.ds((1 - core) * half, half)]
    for copy in gates:
        copy.wait()


def localize(decay_rate, drive_in, gate_in, total):
    batch, length, channels = decay_rate.shape
    big = jax.ShapeDtypeStruct(decay_rate.shape, jnp.float32)
    blocks = jax.ShapeDtypeStruct((batch, length // BLOCK, channels), jnp.float32)
    pair = jax.ShapeDtypeStruct((batch // 2, 2, channels), jnp.float32)
    sems = pltpu.SemaphoreType.DMA((batch * length // PIECE,))
    return pl.pallas_call(
        functools.partial(local_kernel, total),
        out_shape=(big, big, blocks, blocks, jax.ShapeDtypeStruct(gate_in.shape, gate_in.dtype), pair, pair),
        in_specs=[HBM] * 3,
        out_specs=(VMEM,) * 7,
        scratch_shapes=[
            pltpu.VMEM(decay_rate.shape, jnp.float32),
            pltpu.VMEM(drive_in.shape, jnp.bfloat16),
            pltpu.VMEM((batch, 2, channels), jnp.float32),
            pltpu.VMEM((BLOCK, 2 * BLOCK), jnp.bfloat16),
            sems,
            sems,
            pltpu.SemaphoreType.DMA((batch,)),
        ],
        compiler_params=pltpu.CompilerParams(vmem_limit_bytes=20 * MIB),
        cost_estimate=pl.CostEstimate(flops=2_000_000_000, bytes_accessed=8 * MIB, transcendentals=2 * MIB),
        name="localize",
    )(decay_rate, drive_in, gate_in)


def open_kernel(kept_ref, gate_ref, factor_ref):
    batch, length, channels = kept_ref.shape

    def one_piece(n, _):
        at = pl.ds(pl.multiple_of(n * BLOCK, BLOCK), BLOCK)
        for b in range(batch):
            opened = jnp.tanh((0.5 * gate_ref[b, at, :]).astype(jnp.float32)) + 1.0
            factor_ref[b, at, :] = kept_ref[b, at, :] * opened
        return 0

    lax.fori_loop(0, length // BLOCK, one_piece, 0)


def open_gate(kept, gate):
    return pl.pallas_call(
        open_kernel,
        out_shape=jax.ShapeDtypeStruct(kept.shape, jnp.float32),
        in_specs=[VMEM] * 2,
        out_specs=VMEM,
        input_output_aliases={0: 0},
        compiler_params=pltpu.CompilerParams(vmem_limit_bytes=12 * MIB),
        cost_estimate=pl.CostEstimate(flops=8_000_000, bytes_accessed=10 * MIB, transcendentals=MIB),
        name="open_gate",
    )(kept, gate)


def meet_kernel(mine_ref, got_ref, first_ref, every_ref):
    first_core = lax.axis_index("sp_2") == 0
    for p in range(mine_ref.shape[0]):
        mine, got = mine_ref[p], got_ref[p]
        first = jnp.where(first_core, mine, got)
        second = jnp.where(first_core, got, mine)
        first_ref[p] = first
        lost = first[0:1] + second[0:1]
        sums = first[1:2] + jnp.exp2(first[0:1]) * second[1:2]
        for j in range(every_ref.shape[0]):
            every_ref[j, p, 0:1, :] = lost
            every_ref[j, p, 1:2, :] = sums


def meet(mine, got, chips):
    return pl.pallas_call(
        meet_kernel,
        out_shape=(
            jax.ShapeDtypeStruct(mine.shape, jnp.float32),
            jax.ShapeDtypeStruct((chips,) + mine.shape, jnp.float32),
        ),
        in_specs=[VMEM] * 2,
        out_specs=(VMEM,) * 2,
        compiler_params=pltpu.CompilerParams(vmem_limit_bytes=2 * MIB),
        name="meet",
    )(mine, got)


def enter_kernel(every_ref, first_ref, mine_ref, other_ref):
    chips, pairs, _, channels = every_ref.shape
    place = lax.axis_index(CHIPS)
    first_core = lax.axis_index("sp_2") == 0
    for p in range(pairs):
        state = jnp.zeros((1, channels), jnp.float32)
        for j in range(chips):
            kept = jnp.exp2(-jnp.where(j < place, every_ref[j, p, 0:1, :], 0.0))
            state = kept * (state + jnp.where(j < place, every_ref[j, p, 1:2, :], 0.0))
        after = jnp.exp2(-first_ref[p, 0:1, :]) * (state + first_ref[p, 1:2, :])
        mine_ref[p : p + 1, :] = jnp.where(first_core, state, after)
        other_ref[p : p + 1, :] = jnp.where(first_core, after, state)


def entering(every, first):
    chips, pairs, _, channels = every.shape
    out = jax.ShapeDtypeStruct((pairs, channels), jnp.float32)
    return pl.pallas_call(
        enter_kernel,
        out_shape=(out, out),
        in_specs=[VMEM] * 2,
        out_specs=(VMEM,) * 2,
        compiler_params=pltpu.CompilerParams(vmem_limit_bytes=2 * MIB),
        name="entering",
    )(every, first)


def gate_kernel(mine, factor_ref, sum_ref, lost_ref, carry_ref, enter_ref, gain_ref, gated_ref, power_ref):
    half, length, channels = gated_ref.shape
    lane = lax.broadcasted_iota(jnp.int32, (8, length // 8), 1)
    core = lax.axis_index("sp_2")
    start = half * (core if mine else 1 - core)

    for p in range(half):
        b = start + p
        enter = jnp.exp2(-lost_ref[b]) * (enter_ref[pl.ds(p, 1), :] + carry_ref[b])
        gain = jnp.broadcast_to(gain_ref[...], (8, channels))
        power = jnp.zeros((8, length // 8), jnp.float32)
        for k in range(length // BLOCK):
            state = jnp.broadcast_to(enter[k : k + 1, :], (8, channels))
            for j in range(k * BLOCK // 8, (k + 1) * BLOCK // 8):
                at = pl.ds(8 * j, 8)
                gated = factor_ref[b, at, :] * (sum_ref[b, at, :] + state)
                gated_ref[p, at, :] = gated * gain
                power = jnp.where(lane == j, jnp.sum(gated * gated, axis=-1, keepdims=True), power)
        power_ref[p] = power


def gate_and_square(mine, local, enter, gain, name):
    batch, length, channels = local[0].shape
    half = batch // 2
    return pl.pallas_call(
        functools.partial(gate_kernel, mine),
        out_shape=(
            jax.ShapeDtypeStruct((half, length, channels), jnp.float32),
            jax.ShapeDtypeStruct((half, 8, length // 8), jnp.float32),
        ),
        in_specs=[VMEM] * 6,
        out_specs=(VMEM, VMEM),
        compiler_params=pltpu.CompilerParams(vmem_limit_bytes=14 * MIB),
        cost_estimate=pl.CostEstimate(flops=4_000_000, bytes_accessed=6 * MIB, transcendentals=0),
        name=name,
    )(*local, enter, gain)


def scale_kernel(middle, width, mine_ref, got_ref, p0_ref, p1_ref, p2_ref, p3_ref, out_hbm, out, sem):
    half, length, channels = mine_ref.shape
    core = lax.axis_index("sp_2")
    which = [(h, p) for h in range(2) for p in range(half)]

    def copy(h, p, i):
        b = half * (core if h == 0 else 1 - core) + p
        at = pl.ds(i * LEAVING, LEAVING)
        return pltpu.make_async_copy(out.at[h, p, at, :], out_hbm.at[b, at, :], sem.at[(h * half + p) * (length // LEAVING) + i])

    lane = lax.broadcasted_iota(jnp.int32, (8, length // 8), 1)
    scales = []
    for h, p in which:
        power = (p0_ref[h, p] + p1_ref[h, p]) + (p2_ref[h, p] + p3_ref[h, p])
        scales.append(middle * lax.rsqrt(power * (middle * middle / width) + 1e-06))
    for i in range(length // LEAVING):
        for j in range(i * LEAVING // 16, (i + 1) * LEAVING // 16):
            columns = [lane == 2 * j + k for k in range(2)]
            for (h, p), scale in zip(which, scales):
                gated_ref = (mine_ref, got_ref)[h]
                parts = []
                for k, column in enumerate(columns):
                    rows = jnp.sum(jnp.where(column, scale, 0.0), axis=-1, keepdims=True)
                    parts.append(gated_ref[p, pl.ds(16 * j + 8 * k, 8), :] * rows)
                out[h, p, pl.ds(16 * j, 16), :] = jnp.concatenate(parts, axis=0).astype(jnp.bfloat16)
        for h, p in which:
            copy(h, p, i).start()
    for i in range(length // LEAVING):
        for h, p in which:
            copy(h, p, i).wait()


def scale(mine, got, powers, middle, width):
    half, length, channels = mine.shape
    return pl.pallas_call(
        functools.partial(scale_kernel, middle, width),
        out_shape=jax.ShapeDtypeStruct((2 * half, length, channels), jnp.bfloat16),
        in_specs=[VMEM] * 6,
        out_specs=HBM,
        scratch_shapes=[pltpu.VMEM((2,) + mine.shape, jnp.bfloat16), pltpu.SemaphoreType.DMA((2 * half * length // LEAVING,))],
        compiler_params=pltpu.CompilerParams(vmem_limit_bytes=8 * MIB),
        cost_estimate=pl.CostEstimate(flops=8_000_000, bytes_accessed=6 * MIB, transcendentals=0),
        name="scale",
    )(mine, got, *powers)


def shards(decay_rate, drive_in, gate_in, norm_gain):
    total = decay_rate.shape[1] * lax.axis_size(SP)
    parts = lax.axis_size("tp")
    width = decay_rate.shape[2] * parts
    swap = [(0, 1), (1, 0)]
    decay_rate, drive_in, gate_in = (
        pltpu.with_memory_space_constraint(array, pltpu.HBM) for array in (decay_rate, drive_in, gate_in)
    )
    kept, sums, lost, carry, gate, mine, other = localize(decay_rate, drive_in, gate_in, total)
    got = lax.ppermute(other, "sp_2", swap)
    factor = open_gate(kept, gate)
    got, factor = lax.optimization_barrier((got, factor))
    first, every = meet(mine, got, lax.axis_size(CHIPS))
    every = lax.all_to_all(every, CHIPS, 0, 0)
    every, factor, norm_gain = lax.optimization_barrier((every, factor, norm_gain))
    mine, other = entering(every, first)
    got = lax.ppermute(other, "sp_2", swap)
    local, gain = (factor, sums, lost, carry), norm_gain.reshape(1, -1)
    gated_mine, power_mine = gate_and_square(True, local, mine, gain, "gate_mine")
    gated_got, power_got = gate_and_square(False, local, got, gain, "gate_got")
    power = jnp.stack([power_mine, power_got])
    powers = [power] + [lax.ppermute(power, "tp", [(i, i ^ k) for i in range(parts)]) for k in (1, 3, 2)]
    return scale(gated_mine, gated_got, powers, 0.5 * total**-0.5, width)


def solution(mesh):
    torus = Mesh(mesh.devices.reshape(8, 4, 2, mesh.shape["tp"]), ("sp_0", "sp_1", "sp_2", "tp"))
    in_specs = (P(None, SP, "tp"), P(None, SP, "tp"), P(None, SP, "tp"), P("tp"))
    out_specs = P(None, SP, "tp")
    return jax.shard_map(shards, mesh=torus, in_specs=in_specs, out_specs=out_specs, check_vma=False)
```

```python
import functools
import math

import jax
import jax.numpy as jnp
from jax import lax
from jax.experimental import pallas as pl
from jax.experimental.pallas import tpu as pltpu
from jax.sharding import Mesh
from jax.sharding import PartitionSpec as P

SP = ("sp_0", "sp_1", "sp_2")
CHIPS = ("sp_0", "sp_1")
BLOCK = 128
LEAVING = 256
MIB = 1 << 20
VMEM = pl.BlockSpec(memory_space=pltpu.VMEM)
HBM = pl.BlockSpec(memory_space=pltpu.HBM)


def stacked_triangle():
    row = lax.broadcasted_iota(jnp.int32, (BLOCK, 2 * BLOCK), 0)
    col = lax.broadcasted_iota(jnp.int32, (BLOCK, 2 * BLOCK), 1)
    return (row >= col % BLOCK).astype(jnp.bfloat16)


def scan_sequence(total, b, rate, drive, tri_ref, kept_ref, sum_ref, lost_ref, carry_ref):
    length, channels = rate.shape[1:]
    to_log2 = math.log2(math.e) / total
    lost_in = jnp.zeros((1, channels), jnp.float32)
    carry = jnp.zeros((1, channels), jnp.float32)
    for k in range(length // BLOCK):
        at = pl.ds(k * BLOCK, BLOCK)
        rates = rate[b, at, :]
        lost = to_log2 * jnp.dot(tri_ref[:, :BLOCK], rates.astype(jnp.bfloat16), preferred_element_type=jnp.float32)
        kept_ref[b, at, :] = jnp.exp2(-lost)
        drives = drive[b, at, :]
        grown = (jnp.exp2(lost) - 1.0).astype(jnp.bfloat16) * drives
        sums = jnp.dot(tri_ref[...], jnp.concatenate([drives, grown], axis=0), preferred_element_type=jnp.float32)
        sum_ref[b, at, :] = sums
        lost_ref[b, k : k + 1, :] = lost_in
        carry_ref[b, k : k + 1, :] = carry
        carry = carry + jnp.exp2(lost_in) * sums[BLOCK - 1 :, :]
        whole = jnp.sum(rates.reshape(BLOCK // 8, 8, channels), axis=0)
        lost_in = lost_in + to_log2 * jnp.sum(whole, axis=0, keepdims=True)
    return lost_in, carry


def other_kernel(
    total, rate_hbm, drive_hbm, kept_ref, sum_ref, lost_ref, carry_ref, rate, drive, other_ref, tri_ref, rate_sem, drive_sem
):
    batch = rate.shape[0]
    half, core = batch // 2, lax.axis_index("sp_2")
    sets = ((rate_hbm, rate, rate_sem), (drive_hbm, drive, drive_sem))

    def copies(n):
        b = jnp.where(n < half, (1 - core) * half + n, core * half + n - half)
        return [pltpu.make_async_copy(hbm.at[b], vmem.at[b], sems.at[n]) for hbm, vmem, sems in sets]

    for n in range(batch):
        for copy in copies(n):
            copy.start()
    tri_ref[...] = stacked_triangle()

    def one_sequence(n, _):
        for copy in copies(n):
            copy.wait()
        b = (1 - core) * half + n
        lost, carry = scan_sequence(total, b, rate, drive, tri_ref, kept_ref, sum_ref, lost_ref, carry_ref)
        other_ref[n, 0:1, :] = lost
        other_ref[n, 1:2, :] = carry
        return 0

    lax.fori_loop(0, half, one_sequence, 0)
    for n in range(half, batch):
        for copy in copies(n):
            copy.wait()


def scan_other(decay_rate, drive_in, total):
    batch, length, channels = decay_rate.shape
    big = jax.ShapeDtypeStruct(decay_rate.shape, jnp.float32)
    blocks = jax.ShapeDtypeStruct((batch, length // BLOCK, channels), jnp.float32)
    pair = jax.ShapeDtypeStruct((batch // 2, 2, channels), jnp.float32)
    return pl.pallas_call(
        functools.partial(other_kernel, total),
        out_shape=(big, big, blocks, blocks, big, jax.ShapeDtypeStruct(drive_in.shape, drive_in.dtype), pair),
        in_specs=[HBM] * 2,
        out_specs=(VMEM,) * 7,
        scratch_shapes=[
            pltpu.VMEM((BLOCK, 2 * BLOCK), jnp.bfloat16),
            pltpu.SemaphoreType.DMA((batch,)),
            pltpu.SemaphoreType.DMA((batch,)),
        ],
        compiler_params=pltpu.CompilerParams(vmem_limit_bytes=20 * MIB),
        cost_estimate=pl.CostEstimate(flops=1_000_000_000, bytes_accessed=6 * MIB, transcendentals=MIB),
        name="scan_other",
    )(decay_rate, drive_in)


def mine_kernel(
    total,
    rate,
    drive,
    gate_hbm,
    kept_in,
    sum_in,
    lost_in,
    carry_in,
    kept_ref,
    sum_ref,
    lost_ref,
    carry_ref,
    gate_ref,
    mine_ref,
    tri_ref,
    gate_sem,
):
    batch = rate.shape[0]
    half, core = batch // 2, lax.axis_index("sp_2")
    gates = [pltpu.make_async_copy(gate_hbm.at[b], gate_ref.at[b], gate_sem.at[b]) for b in range(batch)]
    for copy in gates:
        copy.start()
    tri_ref[...] = stacked_triangle()

    def one_sequence(n, _):
        b = core * half + n
        lost, carry = scan_sequence(total, b, rate, drive, tri_ref, kept_ref, sum_ref, lost_ref, carry_ref)
        mine_ref[n, 0:1, :] = lost
        mine_ref[n, 1:2, :] = carry
        return 0

    lax.fori_loop(0, half, one_sequence, 0)
    for copy in gates:
        copy.wait()


def scan_mine(rate, drive, gate_in, local, total):
    batch, length, channels = rate.shape
    pair = jax.ShapeDtypeStruct((batch // 2, 2, channels), jnp.float32)
    return pl.pallas_call(
        functools.partial(mine_kernel, total),
        out_shape=(
            *(jax.ShapeDtypeStruct(array.shape, array.dtype) for array in local),
            jax.ShapeDtypeStruct(gate_in.shape, gate_in.dtype),
            pair,
        ),
        in_specs=[VMEM, VMEM, HBM] + [VMEM] * 4,
        out_specs=(VMEM,) * 6,
        scratch_shapes=[pltpu.VMEM((BLOCK, 2 * BLOCK), jnp.bfloat16), pltpu.SemaphoreType.DMA((batch,))],
        input_output_aliases={3: 0, 4: 1, 5: 2, 6: 3},
        compiler_params=pltpu.CompilerParams(vmem_limit_bytes=24 * MIB),
        cost_estimate=pl.CostEstimate(flops=1_000_000_000, bytes_accessed=2 * MIB, transcendentals=MIB),
        name="scan_mine",
    )(rate, drive, gate_in, *local)


def open_kernel(kept_ref, gate_ref, factor_ref):
    batch, length, channels = kept_ref.shape

    def one_piece(n, _):
        at = pl.ds(pl.multiple_of(n * BLOCK, BLOCK), BLOCK)
        for b in range(batch):
            opened = jnp.tanh((0.5 * gate_ref[b, at, :]).astype(jnp.float32)) + 1.0
            factor_ref[b, at, :] = kept_ref[b, at, :] * opened
        return 0

    lax.fori_loop(0, length // BLOCK, one_piece, 0)


def open_gate(kept, gate):
    return pl.pallas_call(
        open_kernel,
        out_shape=jax.ShapeDtypeStruct(kept.shape, jnp.float32),
        in_specs=[VMEM] * 2,
        out_specs=VMEM,
        input_output_aliases={0: 0},
        compiler_params=pltpu.CompilerParams(vmem_limit_bytes=12 * MIB),
        cost_estimate=pl.CostEstimate(flops=8_000_000, bytes_accessed=10 * MIB, transcendentals=MIB),
        name="open_gate",
    )(kept, gate)


def meet_kernel(mine_ref, got_ref, first_ref, every_ref):
    first_core = lax.axis_index("sp_2") == 0
    for p in range(mine_ref.shape[0]):
        mine, got = mine_ref[p], got_ref[p]
        first = jnp.where(first_core, mine, got)
        second = jnp.where(first_core, got, mine)
        first_ref[p] = first
        lost = first[0:1] + second[0:1]
        sums = first[1:2] + jnp.exp2(first[0:1]) * second[1:2]
        for j in range(every_ref.shape[0]):
            every_ref[j, p, 0:1, :] = lost
            every_ref[j, p, 1:2, :] = sums


def meet(mine, got, chips):
    return pl.pallas_call(
        meet_kernel,
        out_shape=(
            jax.ShapeDtypeStruct(mine.shape, jnp.float32),
            jax.ShapeDtypeStruct((chips,) + mine.shape, jnp.float32),
        ),
        in_specs=[VMEM] * 2,
        out_specs=(VMEM,) * 2,
        compiler_params=pltpu.CompilerParams(vmem_limit_bytes=2 * MIB),
        name="meet",
    )(mine, got)


def enter_kernel(every_ref, first_ref, mine_ref, other_ref):
    chips, pairs, _, channels = every_ref.shape
    place = lax.axis_index(CHIPS)
    first_core = lax.axis_index("sp_2") == 0
    for p in range(pairs):
        state = jnp.zeros((1, channels), jnp.float32)
        for j in range(chips):
            kept = jnp.exp2(-jnp.where(j < place, every_ref[j, p, 0:1, :], 0.0))
            state = kept * (state + jnp.where(j < place, every_ref[j, p, 1:2, :], 0.0))
        after = jnp.exp2(-first_ref[p, 0:1, :]) * (state + first_ref[p, 1:2, :])
        mine_ref[p : p + 1, :] = jnp.where(first_core, state, after)
        other_ref[p : p + 1, :] = jnp.where(first_core, after, state)


def entering(every, first):
    chips, pairs, _, channels = every.shape
    out = jax.ShapeDtypeStruct((pairs, channels), jnp.float32)
    return pl.pallas_call(
        enter_kernel,
        out_shape=(out, out),
        in_specs=[VMEM] * 2,
        out_specs=(VMEM,) * 2,
        compiler_params=pltpu.CompilerParams(vmem_limit_bytes=2 * MIB),
        name="entering",
    )(every, first)


def gate_kernel(mine, factor_ref, sum_ref, lost_ref, carry_ref, enter_ref, gated_ref, power_ref):
    half, length, channels = gated_ref.shape
    lane = lax.broadcasted_iota(jnp.int32, (8, length // 8), 1)
    core = lax.axis_index("sp_2")
    start = half * (core if mine else 1 - core)

    for p in range(half):
        b = start + p
        enter = jnp.exp2(-lost_ref[b]) * (enter_ref[pl.ds(p, 1), :] + carry_ref[b])
        power = jnp.zeros((8, length // 8), jnp.float32)
        for k in range(length // BLOCK):
            state = jnp.broadcast_to(enter[k : k + 1, :], (8, channels))
            for j in range(k * BLOCK // 8, (k + 1) * BLOCK // 8):
                at = pl.ds(8 * j, 8)
                gated = factor_ref[b, at, :] * (sum_ref[b, at, :] + state)
                gated_ref[p, at, :] = gated
                power = jnp.where(lane == j, jnp.sum(gated * gated, axis=-1, keepdims=True), power)
        power_ref[p] = power


def gate_and_square(mine, local, enter, name):
    batch, length, channels = local[0].shape
    half = batch // 2
    return pl.pallas_call(
        functools.partial(gate_kernel, mine),
        out_shape=(
            jax.ShapeDtypeStruct((half, length, channels), jnp.float32),
            jax.ShapeDtypeStruct((half, 8, length // 8), jnp.float32),
        ),
        in_specs=[VMEM] * 5,
        out_specs=(VMEM, VMEM),
        compiler_params=pltpu.CompilerParams(vmem_limit_bytes=14 * MIB),
        cost_estimate=pl.CostEstimate(flops=4_000_000, bytes_accessed=6 * MIB, transcendentals=0),
        name=name,
    )(*local, enter)


def scale_kernel(middle, width, mine_ref, got_ref, p0_ref, p1_ref, p2_ref, p3_ref, gain_ref, out_hbm, out, sem):
    half, length, channels = mine_ref.shape
    core = lax.axis_index("sp_2")
    which = [(h, p) for h in range(2) for p in range(half)]

    def copy(h, p, i):
        b = half * (core if h == 0 else 1 - core) + p
        at = pl.ds(i * LEAVING, LEAVING)
        return pltpu.make_async_copy(out.at[h, p, at, :], out_hbm.at[b, at, :], sem.at[(h * half + p) * (length // LEAVING) + i])

    lane = lax.broadcasted_iota(jnp.int32, (8, length // 8), 1)
    gain = jnp.broadcast_to(gain_ref[...], (8, channels))
    scales = []
    for h, p in which:
        power = (p0_ref[h, p] + p1_ref[h, p]) + (p2_ref[h, p] + p3_ref[h, p])
        scales.append(middle * lax.rsqrt(power * (middle * middle / width) + 1e-06))
    for i in range(length // LEAVING):
        for j in range(i * LEAVING // 16, (i + 1) * LEAVING // 16):
            columns = [lane == 2 * j + k for k in range(2)]
            for (h, p), scale in zip(which, scales):
                gated_ref = (mine_ref, got_ref)[h]
                parts = []
                for k, column in enumerate(columns):
                    rows = jnp.sum(jnp.where(column, scale, 0.0), axis=-1, keepdims=True)
                    parts.append(gated_ref[p, pl.ds(16 * j + 8 * k, 8), :] * rows * gain)
                out[h, p, pl.ds(16 * j, 16), :] = jnp.concatenate(parts, axis=0).astype(jnp.bfloat16)
        for h, p in which:
            copy(h, p, i).start()
    for i in range(length // LEAVING):
        for h, p in which:
            copy(h, p, i).wait()


def scale(mine, got, powers, gain, middle, width):
    half, length, channels = mine.shape
    return pl.pallas_call(
        functools.partial(scale_kernel, middle, width),
        out_shape=jax.ShapeDtypeStruct((2 * half, length, channels), jnp.bfloat16),
        in_specs=[VMEM] * 7,
        out_specs=HBM,
        scratch_shapes=[pltpu.VMEM((2,) + mine.shape, jnp.bfloat16), pltpu.SemaphoreType.DMA((2 * half * length // LEAVING,))],
        compiler_params=pltpu.CompilerParams(vmem_limit_bytes=8 * MIB),
        cost_estimate=pl.CostEstimate(flops=8_000_000, bytes_accessed=6 * MIB, transcendentals=0),
        name="scale",
    )(mine, got, *powers, gain.reshape(1, channels))


def shards(decay_rate, drive_in, gate_in, norm_gain):
    total = decay_rate.shape[1] * lax.axis_size(SP)
    parts = lax.axis_size("tp")
    width = decay_rate.shape[2] * parts
    swap = [(0, 1), (1, 0)]
    decay_rate, drive_in, gate_in = (
        pltpu.with_memory_space_constraint(array, pltpu.HBM) for array in (decay_rate, drive_in, gate_in)
    )
    *local, rate, drive, other = scan_other(decay_rate, drive_in, total)
    got = lax.ppermute(other, "sp_2", swap)
    kept, sums, lost, carry, gate, mine = scan_mine(rate, drive, gate_in, local, total)
    first, every = meet(mine, got, lax.axis_size(CHIPS))
    every = lax.all_to_all(every, CHIPS, 0, 0)
    every, kept, gate, norm_gain = lax.optimization_barrier((every, kept, gate, norm_gain))
    mine, other = entering(every, first)
    got = lax.ppermute(other, "sp_2", swap)
    factor = open_gate(kept, gate)
    local = (factor, sums, lost, carry)
    gated_mine, power_mine = gate_and_square(True, local, mine, "gate_mine")
    gated_got, power_got = gate_and_square(False, local, got, "gate_got")
    power = jnp.stack([power_mine, power_got])
    powers = [power] + [lax.ppermute(power, "tp", [(i, i ^ k) for i in range(parts)]) for k in (1, 3, 2)]
    return scale(gated_mine, gated_got, powers, norm_gain, 0.5 * total**-0.5, width)


def solution(mesh):
    torus = Mesh(mesh.devices.reshape(8, 4, 2, mesh.shape["tp"]), ("sp_0", "sp_1", "sp_2", "tp"))
    in_specs = (P(None, SP, "tp"), P(None, SP, "tp"), P(None, SP, "tp"), P("tp"))
    out_specs = P(None, SP, "tp")
    return jax.shard_map(shards, mesh=torus, in_specs=in_specs, out_specs=out_specs, check_vma=False)
```

```python
import functools
import math

import jax
import jax.numpy as jnp
from jax import lax
from jax.experimental import pallas as pl
from jax.experimental.pallas import tpu as pltpu
from jax.sharding import Mesh
from jax.sharding import PartitionSpec as P

SP = ("sp_0", "sp_1", "sp_2")
CHIPS = ("sp_0", "sp_1")
BLOCK = 128
LEAVING = 256
MIB = 1 << 20
VMEM = pl.BlockSpec(memory_space=pltpu.VMEM)
HBM = pl.BlockSpec(memory_space=pltpu.HBM)


def stacked_triangle():
    row = lax.broadcasted_iota(jnp.int32, (BLOCK, 2 * BLOCK), 0)
    col = lax.broadcasted_iota(jnp.int32, (BLOCK, 2 * BLOCK), 1)
    return (row >= col % BLOCK).astype(jnp.bfloat16)


def scan_sequence(total, b, rate, drive, tri_ref, kept_ref, sum_ref, lost_ref, carry_ref):
    length, channels = rate.shape[1:]
    to_log2 = math.log2(math.e) / total
    lost_in = jnp.zeros((1, channels), jnp.float32)
    carry = jnp.zeros((1, channels), jnp.float32)
    for k in range(length // BLOCK):
        at = pl.ds(k * BLOCK, BLOCK)
        rates = rate[b, at, :]
        lost = to_log2 * jnp.dot(tri_ref[:, :BLOCK], rates.astype(jnp.bfloat16), preferred_element_type=jnp.float32)
        kept_ref[b, at, :] = jnp.exp2(-lost)
        drives = drive[b, at, :]
        grown = (jnp.exp2(lost) - 1.0).astype(jnp.bfloat16) * drives
        sums = jnp.dot(tri_ref[...], jnp.concatenate([drives, grown], axis=0), preferred_element_type=jnp.float32)
        sum_ref[b, at, :] = sums
        lost_ref[b, k : k + 1, :] = lost_in
        carry_ref[b, k : k + 1, :] = carry
        carry = carry + jnp.exp2(lost_in) * sums[BLOCK - 1 :, :]
        whole = jnp.sum(rates.reshape(BLOCK // 8, 8, channels), axis=0)
        lost_in = lost_in + to_log2 * jnp.sum(whole, axis=0, keepdims=True)
    return lost_in, carry


def other_kernel(
    total, rate_hbm, drive_hbm, kept_ref, sum_ref, lost_ref, carry_ref, rate, drive, other_ref, tri_ref, rate_sem, drive_sem
):
    batch = rate.shape[0]
    half, core = batch // 2, lax.axis_index("sp_2")
    sets = ((rate_hbm, rate, rate_sem), (drive_hbm, drive, drive_sem))

    def copies(n):
        b = jnp.where(n < half, (1 - core) * half + n, core * half + n - half)
        return [pltpu.make_async_copy(hbm.at[b], vmem.at[b], sems.at[n]) for hbm, vmem, sems in sets]

    for n in range(batch):
        for copy in copies(n):
            copy.start()
    tri_ref[...] = stacked_triangle()

    def one_sequence(n, _):
        for copy in copies(n):
            copy.wait()
        b = (1 - core) * half + n
        lost, carry = scan_sequence(total, b, rate, drive, tri_ref, kept_ref, sum_ref, lost_ref, carry_ref)
        other_ref[n, 0:1, :] = lost
        other_ref[n, 1:2, :] = carry
        return 0

    lax.fori_loop(0, half, one_sequence, 0)
    for n in range(half, batch):
        for copy in copies(n):
            copy.wait()


def scan_other(decay_rate, drive_in, total):
    batch, length, channels = decay_rate.shape
    big = jax.ShapeDtypeStruct(decay_rate.shape, jnp.float32)
    blocks = jax.ShapeDtypeStruct((batch, length // BLOCK, channels), jnp.float32)
    pair = jax.ShapeDtypeStruct((batch // 2, 2, channels), jnp.float32)
    return pl.pallas_call(
        functools.partial(other_kernel, total),
        out_shape=(big, big, blocks, blocks, big, jax.ShapeDtypeStruct(drive_in.shape, drive_in.dtype), pair),
        in_specs=[HBM] * 2,
        out_specs=(VMEM,) * 7,
        scratch_shapes=[
            pltpu.VMEM((BLOCK, 2 * BLOCK), jnp.bfloat16),
            pltpu.SemaphoreType.DMA((batch,)),
            pltpu.SemaphoreType.DMA((batch,)),
        ],
        compiler_params=pltpu.CompilerParams(vmem_limit_bytes=20 * MIB),
        cost_estimate=pl.CostEstimate(flops=1_000_000_000, bytes_accessed=6 * MIB, transcendentals=MIB),
        name="scan_other",
    )(decay_rate, drive_in)


def mine_kernel(
    total,
    rate,
    drive,
    gate_hbm,
    kept_in,
    sum_in,
    lost_in,
    carry_in,
    kept_ref,
    sum_ref,
    lost_ref,
    carry_ref,
    gate_ref,
    mine_ref,
    tri_ref,
    gate_sem,
):
    batch = rate.shape[0]
    half, core = batch // 2, lax.axis_index("sp_2")
    gates = [pltpu.make_async_copy(gate_hbm.at[b], gate_ref.at[b], gate_sem.at[b]) for b in range(batch)]
    for copy in gates:
        copy.start()
    tri_ref[...] = stacked_triangle()

    def one_sequence(n, _):
        b = core * half + n
        lost, carry = scan_sequence(total, b, rate, drive, tri_ref, kept_ref, sum_ref, lost_ref, carry_ref)
        mine_ref[n, 0:1, :] = lost
        mine_ref[n, 1:2, :] = carry
        return 0

    lax.fori_loop(0, half, one_sequence, 0)
    for copy in gates:
        copy.wait()


def scan_mine(rate, drive, gate_in, local, total):
    batch, length, channels = rate.shape
    pair = jax.ShapeDtypeStruct((batch // 2, 2, channels), jnp.float32)
    return pl.pallas_call(
        functools.partial(mine_kernel, total),
        out_shape=(
            *(jax.ShapeDtypeStruct(array.shape, array.dtype) for array in local),
            jax.ShapeDtypeStruct(gate_in.shape, gate_in.dtype),
            pair,
        ),
        in_specs=[VMEM, VMEM, HBM] + [VMEM] * 4,
        out_specs=(VMEM,) * 6,
        scratch_shapes=[pltpu.VMEM((BLOCK, 2 * BLOCK), jnp.bfloat16), pltpu.SemaphoreType.DMA((batch,))],
        input_output_aliases={3: 0, 4: 1, 5: 2, 6: 3},
        compiler_params=pltpu.CompilerParams(vmem_limit_bytes=24 * MIB),
        cost_estimate=pl.CostEstimate(flops=1_000_000_000, bytes_accessed=2 * MIB, transcendentals=MIB),
        name="scan_mine",
    )(rate, drive, gate_in, *local)


def open_kernel(core, kept_ref, gate_ref, factor_ref):
    batch, length, channels = kept_ref.shape

    def one_piece(n, _):
        at = pl.ds(pl.multiple_of(n * BLOCK, BLOCK), BLOCK)
        for b in range(batch):
            opened = jnp.tanh((0.5 * gate_ref[b, at, :]).astype(jnp.float32)) + 1.0
            factor_ref[b, at, :] = kept_ref[b, at, :] * opened
        return 0

    @pl.when(lax.axis_index("sp_2") == core)
    def _():
        lax.fori_loop(0, length // BLOCK, one_piece, 0)


def open_gate(core, kept, gate):
    return pl.pallas_call(
        functools.partial(open_kernel, core),
        out_shape=jax.ShapeDtypeStruct(kept.shape, jnp.float32),
        in_specs=[VMEM] * 2,
        out_specs=VMEM,
        input_output_aliases={0: 0},
        compiler_params=pltpu.CompilerParams(vmem_limit_bytes=12 * MIB),
        cost_estimate=pl.CostEstimate(flops=8_000_000, bytes_accessed=10 * MIB, transcendentals=MIB),
        name=f"open_gate_{core}",
    )(kept, gate)


def meet_kernel(mine_ref, got_ref, first_ref, every_ref):
    first_core = lax.axis_index("sp_2") == 0
    for p in range(mine_ref.shape[0]):
        mine, got = mine_ref[p], got_ref[p]
        first = jnp.where(first_core, mine, got)
        second = jnp.where(first_core, got, mine)
        first_ref[p] = first
        lost = first[0:1] + second[0:1]
        sums = first[1:2] + jnp.exp2(first[0:1]) * second[1:2]
        for j in range(every_ref.shape[0]):
            every_ref[j, p, 0:1, :] = lost
            every_ref[j, p, 1:2, :] = sums


def meet(mine, got, chips):
    return pl.pallas_call(
        meet_kernel,
        out_shape=(
            jax.ShapeDtypeStruct(mine.shape, jnp.float32),
            jax.ShapeDtypeStruct((chips,) + mine.shape, jnp.float32),
        ),
        in_specs=[VMEM] * 2,
        out_specs=(VMEM,) * 2,
        compiler_params=pltpu.CompilerParams(vmem_limit_bytes=2 * MIB),
        name="meet",
    )(mine, got)


def enter_kernel(every_ref, first_ref, mine_ref, other_ref):
    chips, pairs, _, channels = every_ref.shape
    place = lax.axis_index(CHIPS)
    first_core = lax.axis_index("sp_2") == 0
    for p in range(pairs):
        state = jnp.zeros((1, channels), jnp.float32)
        for j in range(chips):
            kept = jnp.exp2(-jnp.where(j < place, every_ref[j, p, 0:1, :], 0.0))
            state = kept * (state + jnp.where(j < place, every_ref[j, p, 1:2, :], 0.0))
        after = jnp.exp2(-first_ref[p, 0:1, :]) * (state + first_ref[p, 1:2, :])
        mine_ref[p : p + 1, :] = jnp.where(first_core, state, after)
        other_ref[p : p + 1, :] = jnp.where(first_core, after, state)


def entering(every, first):
    chips, pairs, _, channels = every.shape
    out = jax.ShapeDtypeStruct((pairs, channels), jnp.float32)
    return pl.pallas_call(
        enter_kernel,
        out_shape=(out, out),
        in_specs=[VMEM] * 2,
        out_specs=(VMEM,) * 2,
        compiler_params=pltpu.CompilerParams(vmem_limit_bytes=2 * MIB),
        name="entering",
    )(every, first)


def gate_kernel(mine, factor_ref, sum_ref, lost_ref, carry_ref, enter_ref, gated_ref, power_ref):
    half, length, channels = gated_ref.shape
    lane = lax.broadcasted_iota(jnp.int32, (8, length // 8), 1)
    core = lax.axis_index("sp_2")
    start = half * (core if mine else 1 - core)

    for p in range(half):
        b = start + p
        enter = jnp.exp2(-lost_ref[b]) * (enter_ref[pl.ds(p, 1), :] + carry_ref[b])
        power = jnp.zeros((8, length // 8), jnp.float32)
        for k in range(length // BLOCK):
            state = jnp.broadcast_to(enter[k : k + 1, :], (8, channels))
            for j in range(k * BLOCK // 8, (k + 1) * BLOCK // 8):
                at = pl.ds(8 * j, 8)
                gated = factor_ref[b, at, :] * (sum_ref[b, at, :] + state)
                gated_ref[p, at, :] = gated
                power = jnp.where(lane == j, jnp.sum(gated * gated, axis=-1, keepdims=True), power)
        power_ref[p] = power


def gate_and_square(mine, local, enter, name):
    batch, length, channels = local[0].shape
    half = batch // 2
    return pl.pallas_call(
        functools.partial(gate_kernel, mine),
        out_shape=(
            jax.ShapeDtypeStruct((half, length, channels), jnp.float32),
            jax.ShapeDtypeStruct((half, 8, length // 8), jnp.float32),
        ),
        in_specs=[VMEM] * 5,
        out_specs=(VMEM, VMEM),
        compiler_params=pltpu.CompilerParams(vmem_limit_bytes=14 * MIB),
        cost_estimate=pl.CostEstimate(flops=4_000_000, bytes_accessed=6 * MIB, transcendentals=0),
        name=name,
    )(*local, enter)


def scale_kernel(middle, width, mine_ref, got_ref, p0_ref, p1_ref, p2_ref, p3_ref, gain_ref, out_hbm, out, sem):
    half, length, channels = mine_ref.shape
    core = lax.axis_index("sp_2")
    which = [(h, p) for h in range(2) for p in range(half)]

    def copy(h, p, i):
        b = half * (core if h == 0 else 1 - core) + p
        at = pl.ds(i * LEAVING, LEAVING)
        return pltpu.make_async_copy(out.at[h, p, at, :], out_hbm.at[b, at, :], sem.at[(h * half + p) * (length // LEAVING) + i])

    lane = lax.broadcasted_iota(jnp.int32, (8, length // 8), 1)
    gain = jnp.broadcast_to(gain_ref[...], (8, channels))
    scales = []
    for h, p in which:
        power = (p0_ref[h, p] + p1_ref[h, p]) + (p2_ref[h, p] + p3_ref[h, p])
        scales.append(middle * lax.rsqrt(power * (middle * middle / width) + 1e-06))
    for i in range(length // LEAVING):
        for j in range(i * LEAVING // 16, (i + 1) * LEAVING // 16):
            columns = [lane == 2 * j + k for k in range(2)]
            for (h, p), scale in zip(which, scales):
                gated_ref = (mine_ref, got_ref)[h]
                parts = []
                for k, column in enumerate(columns):
                    rows = jnp.sum(jnp.where(column, scale, 0.0), axis=-1, keepdims=True)
                    parts.append(gated_ref[p, pl.ds(16 * j + 8 * k, 8), :] * rows * gain)
                out[h, p, pl.ds(16 * j, 16), :] = jnp.concatenate(parts, axis=0).astype(jnp.bfloat16)
        for h, p in which:
            copy(h, p, i).start()
    for i in range(length // LEAVING):
        for h, p in which:
            copy(h, p, i).wait()


def scale(mine, got, powers, gain, middle, width):
    half, length, channels = mine.shape
    return pl.pallas_call(
        functools.partial(scale_kernel, middle, width),
        out_shape=jax.ShapeDtypeStruct((2 * half, length, channels), jnp.bfloat16),
        in_specs=[VMEM] * 7,
        out_specs=HBM,
        scratch_shapes=[pltpu.VMEM((2,) + mine.shape, jnp.bfloat16), pltpu.SemaphoreType.DMA((2 * half * length // LEAVING,))],
        compiler_params=pltpu.CompilerParams(vmem_limit_bytes=8 * MIB),
        cost_estimate=pl.CostEstimate(flops=8_000_000, bytes_accessed=6 * MIB, transcendentals=0),
        name="scale",
    )(mine, got, *powers, gain.reshape(1, channels))


def shards(decay_rate, drive_in, gate_in, norm_gain):
    total = decay_rate.shape[1] * lax.axis_size(SP)
    parts = lax.axis_size("tp")
    width = decay_rate.shape[2] * parts
    swap = [(0, 1), (1, 0)]
    decay_rate, drive_in, gate_in = (
        pltpu.with_memory_space_constraint(array, pltpu.HBM) for array in (decay_rate, drive_in, gate_in)
    )
    *local, rate, drive, other = scan_other(decay_rate, drive_in, total)
    got = lax.ppermute(other, "sp_2", swap)
    kept, sums, lost, carry, gate, mine = scan_mine(rate, drive, gate_in, local, total)
    first, every = meet(mine, got, lax.axis_size(CHIPS))
    every = lax.all_to_all(every, CHIPS, 0, 0)
    every, kept, gate, norm_gain = lax.optimization_barrier((every, kept, gate, norm_gain))
    mine, other = entering(every, first)
    kept = open_gate(1, kept, gate)
    other, kept = lax.optimization_barrier((other, kept))
    got = lax.ppermute(other, "sp_2", swap)
    factor = open_gate(0, kept, gate)
    local = (factor, sums, lost, carry)
    gated_mine, power_mine = gate_and_square(True, local, mine, "gate_mine")
    gated_got, power_got = gate_and_square(False, local, got, "gate_got")
    power = jnp.stack([power_mine, power_got])
    powers = [power] + [lax.ppermute(power, "tp", [(i, i ^ k) for i in range(parts)]) for k in (1, 3, 2)]
    return scale(gated_mine, gated_got, powers, norm_gain, 0.5 * total**-0.5, width)


def solution(mesh):
    torus = Mesh(mesh.devices.reshape(8, 4, 2, mesh.shape["tp"]), ("sp_0", "sp_1", "sp_2", "tp"))
    in_specs = (P(None, SP, "tp"), P(None, SP, "tp"), P(None, SP, "tp"), P("tp"))
    out_specs = P(None, SP, "tp")
    return jax.shard_map(shards, mesh=torus, in_specs=in_specs, out_specs=out_specs, check_vma=False)
```
